128 devices in a mesh: replica: 1, data: 128 (over z, y, x, core).
Axes of the slice: x: 4, y: 4, z: 4, core: 2. Of those that a mesh axis runs over, the one named last changes fastest.
Arguments:
- q_hidden: bfloat16 [512, 32, 768], P(('replica', 'data'))
- d_hidden: bfloat16 [512, 180, 768], P(('replica', 'data'))
- w_proj: bfloat16 [768, 128], replicated
- q_mask: int32 [512, 32], P(('replica', 'data'))
- d_mask: int32 [512, 180], P(('replica', 'data'))
- temperature: float32 [], replicated
Outputs:
- output 1: float32 [512], P(('replica', 'data'))
- output 2: float32 [512], P(('replica', 'data'))
- output 3: float32 [1], P('replica')
All inputs are finite; a program needn't handle non-finite values.
Results may differ from the reference program's by a relative error of at most 0.001.
Values are sent between devices in bfloat16 or wider.
A program may use at most 1 GiB of HBM per device.

```python
import jax
import jax.numpy as jnp
from jax import lax

HIDDEN = 768
PROJ_DIM = 128
Q_LEN = 32
DOC_LEN = 180
GROUP_PAIRS = 512


def setup_inputs(seed: int = 0, part: int = 0) -> dict:
    root_key = jax.random.key(seed)
    shared_keys = jax.random.split(jax.random.fold_in(root_key, 1), 2)
    part_keys = jax.random.split(jax.random.fold_in(jax.random.fold_in(root_key, 2), part), 6)
    w_proj = jax.random.normal(shared_keys[0], (HIDDEN, PROJ_DIM), jnp.float32) * HIDDEN ** -0.5
    temperature = jax.random.uniform(shared_keys[1], (), jnp.float32, 0.12, 0.2) * Q_LEN
    common = jax.random.normal(part_keys[0], (HIDDEN,), jnp.float32)
    topics = jax.random.normal(part_keys[1], (GROUP_PAIRS, HIDDEN), jnp.float32)
    q_noise = jax.random.normal(part_keys[2], (GROUP_PAIRS, Q_LEN, HIDDEN), jnp.float32)
    d_noise = jax.random.normal(part_keys[3], (GROUP_PAIRS, DOC_LEN, HIDDEN), jnp.float32)
    q_lens = jax.random.randint(part_keys[4], (GROUP_PAIRS,), Q_LEN // 2, Q_LEN + 1)
    d_lens = jax.random.randint(part_keys[5], (GROUP_PAIRS,), DOC_LEN // 4, DOC_LEN + 1)
    q_mask = (jnp.arange(Q_LEN)[None, :] < q_lens[:, None]).astype(jnp.int32)
    d_mask = (jnp.arange(DOC_LEN)[None, :] < d_lens[:, None]).astype(jnp.int32)
    q_real = common + topics[:, None, :] + q_noise
    q_pad = common + 2.0 * jnp.roll(topics, 1, axis=0)[:, None, :] + 0.5 * q_noise
    d_real = common + topics[:, None, :] + d_noise
    d_pad = 4.0 * common + 0.5 * d_noise
    q_hidden = jnp.where(q_mask[:, :, None] == 1, q_real, q_pad).astype(jnp.bfloat16)
    d_hidden = jnp.where(d_mask[:, :, None] == 1, d_real, d_pad).astype(jnp.bfloat16)
    return {'q_hidden': q_hidden, 'd_hidden': d_hidden, 'w_proj': w_proj.astype(jnp.bfloat16), 'q_mask': q_mask, 'd_mask': d_mask, 'temperature': temperature}


def project(hidden, w_proj):
    flat_rows = hidden.reshape(-1, hidden.shape[-1])
    raw_proj = jnp.dot(flat_rows, w_proj, preferred_element_type=jnp.float32)
    unit_vecs = raw_proj / jnp.sqrt(jnp.sum(raw_proj * raw_proj, axis=-1, keepdims=True))
    return unit_vecs.astype(jnp.bfloat16).reshape(hidden.shape[:-1] + (w_proj.shape[1],))


def reference(q_hidden, d_hidden, w_proj, q_mask, d_mask, temperature):
    q_vecs = project(q_hidden, w_proj).astype(jnp.float32)
    p_vecs = project(d_hidden, w_proj).astype(jnp.float32)
    doc_valid = d_mask == 1

    def score_row(row_args):
        q_row, q_valid = row_args
        sim_vals = jnp.einsum('tk,jsk->tjs', q_row, p_vecs)
        best_sim = jnp.max(jnp.where(doc_valid[None, :, :], sim_vals, -jnp.inf), axis=2)
        return jnp.sum(jnp.where(q_valid[:, None] == 1, best_sim, 0.0), axis=0)

    scores = lax.map(score_row, (q_vecs, q_mask))
    logits = scores / temperature
    pos_logit = jnp.diagonal(logits)
    loss_query = jax.nn.logsumexp(logits, axis=1) - pos_logit
    loss_doc = jax.nn.logsumexp(logits, axis=0) - pos_logit
    loss_mean = (0.5 * jnp.mean(loss_query + loss_doc)).reshape(1)
    return loss_query, loss_doc, loss_mean
```

```python
import functools
import jax
import jax.numpy as jnp
from jax import lax
from jax.experimental import pallas as pl
from jax.experimental.pallas import tpu as pltpu
from jax.sharding import PartitionSpec as P

F32 = jnp.float32
BF16 = jnp.bfloat16
MESH = pl.DeviceIdType.MESH
NZ, NY, NX, NC = 4, 4, 4, 2
DPAD = 184


def unit_rows(raw):
    return raw / jnp.sqrt(jnp.sum(raw * raw, axis=-1, keepdims=True))


def kernel(q_hbm, d_hbm, w_hbm, qm_hbm, dm_hbm, temp_ref, lq_ref, ld_ref, lm_ref,
           qh, dh, w, qm, dm, qbuf, dbuf, best, rowbuf, colbuf, row2, col2,
           lsem, qs, qr, ds_, dr, ps, pr, rs, rr, cs, cr, rs2, rr2, cs2, cr2):
    me = lax.axis_index('data')
    c = lax.rem(me, 2)
    x = lax.rem(me // 2, 4)
    y = lax.rem(me // 8, 4)
    z = me // 32

    def dev(z_, y_, x_, c_):
        return {'data': ((z_ * 4 + y_) * 4 + x_) * 2 + c_}

    def plane(r):
        return lax.rem(z + r // 4, 4), lax.rem(y + r % 4, 4)

    def plane_back(r):
        return lax.rem(z + 4 - r // 4, 4), lax.rem(y + 4 - r % 4, 4)

    def line(r):
        return lax.rem(x + r // 2, 4), lax.rem(c + r % 2, 2)

    def line_back(r):
        return lax.rem(x + 4 - r // 2, 4), lax.rem(c + r % 2, 2)

    loads = [pltpu.make_async_copy(w_hbm, w, lsem.at[0]),
             pltpu.make_async_copy(q_hbm, qh, lsem.at[1]),
             pltpu.make_async_copy(qm_hbm, qm, lsem.at[2]),
             pltpu.make_async_copy(dm_hbm, dm, lsem.at[3])]
    loads += [pltpu.make_async_copy(d_hbm.at[j], dh.at[j], lsem.at[4 + j]) for j in range(4)]
    for cp in loads:
        cp.start()

    barrier = pltpu.get_barrier_semaphore()
    for r in range(1, 16):
        zz, yy = plane(r)
        pl.semaphore_signal(barrier, inc=1, device_id=dev(zz, yy, x, c), device_id_type=MESH)
    for r in range(1, 8):
        xx, cc = line(r)
        pl.semaphore_signal(barrier, inc=1, device_id=dev(z, y, xx, cc), device_id_type=MESH)

    for cp in loads[:4]:
        cp.wait()
    q_raw = jnp.dot(qh[...].reshape(128, 768), w[...], preferred_element_type=F32)
    q_col = jnp.transpose(jnp.concatenate([qm[...].astype(F32), jnp.zeros((4, 32), F32)], axis=0))
    q_valid = jnp.concatenate([q_col[:, i:i + 1] for i in range(4)], axis=0)
    q_unit = jnp.where(q_valid == 1.0, unit_rows(q_raw), 0.0).astype(BF16)
    my_slot = z * 4 + y
    qbuf[my_slot] = q_unit

    pl.semaphore_wait(barrier, 22)

    def q_copy(r):
        zz, yy = plane_back(r)
        return pltpu.make_async_remote_copy(qbuf.at[my_slot], qbuf.at[my_slot], qs.at[r], qr.at[r],
                                            device_id=dev(zz, yy, x, c), device_id_type=MESH)

    q_order = [1, 3, 4, 12, 5, 15, 7, 13, 2, 8, 6, 9, 14, 11, 10]
    for r in q_order:
        q_copy(r).start()

    d_col = jnp.transpose(jnp.concatenate([dm[...].astype(F32), jnp.zeros((4, 180), F32)], axis=0))
    pos = lax.broadcasted_iota(jnp.int32, (180, 1), 0)

    def piece(xx, cc, h):
        return dbuf.at[xx, cc, h]

    def d_copy(xx, cc, h, to, ssem, rsem):
        return pltpu.make_async_remote_copy(piece(xx, cc, h), piece(xx, cc, h), ssem, rsem,
                                            device_id=to, device_id_type=MESH)

    xr, xl, xo, cp_ = lax.rem(x + 1, 4), lax.rem(x + 3, 4), lax.rem(x + 2, 4), 1 - c
    right, left, partner = dev(z, y, xr, c), dev(z, y, xl, c), dev(z, y, x, cp_)
    sends = []

    def send(cp):
        cp.start()
        sends.append(cp)

    for h in range(2):
        parts = []
        for j in (2 * h, 2 * h + 1):
            loads[4 + j].wait()
            u = unit_rows(jnp.dot(dh[j], w[...], preferred_element_type=F32))
            valid = d_col[:, j:j + 1] == 1.0
            first = jnp.min(jnp.where(valid, pos, 1000), axis=0, keepdims=True)
            vec = jnp.sum(jnp.where(pos == first, u, 0.0), axis=0, keepdims=True)
            u = jnp.where(valid, u, vec)
            parts += [u, jnp.broadcast_to(vec, (DPAD - 180, 128))]
        dbuf[x, c, h] = jnp.concatenate(parts, axis=0).astype(BF16)
        send(d_copy(x, c, h, right, ds_.at[h], dr.at[h]))
        send(d_copy(x, c, h, left, ds_.at[2 + h], dr.at[2 + h]))
        send(d_copy(x, c, h, partner, ps.at[h], pr.at[h]))

    def wait_ici(i):
        xx, h = [(xl, 0), (xl, 1), (xr, 0), (xr, 1), (xo, 0), (xo, 1)][i]
        d_copy(xx, c, h, right, ds_.at[i], dr.at[i]).wait_recv()
        if i == 0:
            send(d_copy(xl, c, 0, right, ds_.at[4], dr.at[4]))
        if i == 3:
            send(d_copy(xr, c, 1, left, ds_.at[5], dr.at[5]))
        send(d_copy(xx, c, h, partner, ps.at[2 + i], pr.at[2 + i]))

    def wait_partner(i):
        xx, h = [(x, 0), (x, 1), (xl, 0), (xl, 1), (xr, 0), (xr, 1), (xo, 0), (xo, 1)][i]
        d_copy(xx, cp_, h, partner, ps.at[i], pr.at[i]).wait_recv()

    def wait_q(r):
        q_copy(r).wait_recv()

    def unit(xx, k):
        r = 2 * k
        slots = []
        for rr_ in (r, r + 1):
            zz, yy = lax.rem(z + rr_ // 4, 4), lax.rem(y + lax.rem(rr_, 4), 4)
            slots.append(zz * 4 + yy)
        rhs = jnp.concatenate([qbuf[s] for s in slots], axis=0)
        lhs = dbuf[xx].reshape(8 * DPAD, 128)
        sim = lax.dot_general(lhs, rhs, (((1,), (1,)), ((), ())), preferred_element_type=F32)
        top = jnp.max(sim.reshape(8, DPAD, 256), axis=1)
        row = pl.ds(pl.multiple_of(xx * 8, 8), 8)
        for i in range(2):
            best[row, pl.ds(pl.multiple_of(slots[i] * 128, 128), 128)] = top[:, i * 128:(i + 1) * 128]

    wait_partner(0)
    wait_partner(1)

    def q_loop(lo, hi):
        def body(k, carry):
            @pl.when(k > 0)
            def _():
                q_copy_dyn(2 * k).wait_recv()
            q_copy_dyn(2 * k + 1).wait_recv()
            unit(x, k)
            return carry
        lax.fori_loop(lo, hi, body, 0)

    def q_copy_dyn(r):
        zz, yy = lax.rem(z + 4 - r // 4, 4), lax.rem(y + 4 - lax.rem(r, 4), 4)
        return pltpu.make_async_remote_copy(qbuf.at[my_slot], qbuf.at[my_slot], qs.at[r], qr.at[r],
                                            device_id=dev(zz, yy, x, c), device_id_type=MESH)

    q_loop(0, 2)
    wait_ici(0)
    wait_ici(2)
    q_loop(2, 4)
    wait_ici(1)
    wait_ici(3)
    q_loop(4, 8)

    def d_loop(xx):
        def body(k, carry):
            unit(xx, k)
            return carry
        lax.fori_loop(0, 8, body, 0)

    wait_partner(2)
    wait_partner(3)
    d_loop(xl)
    wait_ici(4)
    wait_ici(5)
    wait_partner(4)
    wait_partner(5)
    d_loop(xr)
    wait_partner(6)
    wait_partner(7)
    d_loop(xo)

    b = best[...]
    hi = b.astype(BF16)
    rest = b - hi.astype(F32)
    mid = rest.astype(BF16)
    low = (rest - mid.astype(F32)).astype(BF16)
    tok = lax.broadcasted_iota(jnp.int32, (2048, 128), 0) // 32
    pick = (tok == lax.broadcasted_iota(jnp.int32, (2048, 128), 1)).astype(F32).astype(BF16)
    sums = jnp.dot(jnp.concatenate([hi, mid, low], axis=0), pick, preferred_element_type=F32)
    logits = ((sums[0:32] + sums[32:64]) + sums[64:96]) / temp_ref[0]
    lane = lax.broadcasted_iota(jnp.int32, (32, 128), 1)
    sub = lax.broadcasted_iota(jnp.int32, (32, 128), 0)
    lane1 = lax.broadcasted_iota(jnp.int32, (1, 128), 1)
    own_row = (sub // 4) == (x * 2 + c)
    own = own_row & (lane - my_slot * 4 == lax.rem(sub, 4))
    pos_q = jnp.sum(jnp.where(own, logits, 0.0), axis=0, keepdims=True)
    pos_total = jnp.sum(pos_q, axis=1, keepdims=True)
    m_row = jnp.max(logits, axis=0, keepdims=True)
    l_row = jnp.sum(jnp.exp(logits - m_row), axis=0, keepdims=True)
    qlane = lane < 64
    m_col = jnp.max(jnp.where(qlane, logits, -jnp.inf), axis=1, keepdims=True)
    l_col = jnp.sum(jnp.where(qlane, jnp.exp(logits - m_col), 0.0), axis=1, keepdims=True)
    m_colr = jnp.sum(jnp.where(sub == lane, m_col, 0.0), axis=0, keepdims=True)
    l_colr = jnp.sum(jnp.where(sub == lane - 32, l_col, 0.0), axis=0, keepdims=True)
    rowbuf[my_slot] = jnp.where(lane1 < 64, m_row, pltpu.roll(l_row, 64, 1))
    my_line = x * 2 + c
    colbuf[my_line] = jnp.where(lane1 == 64, pos_total, m_colr + l_colr)

    def plane_copy(buf, r, ss, rs_):
        zz, yy = plane_back(r)
        return pltpu.make_async_remote_copy(buf.at[my_slot], buf.at[my_slot], ss.at[r], rs_.at[r],
                                            device_id=dev(zz, yy, x, c), device_id_type=MESH)

    def line_copy(buf, r, ss, rs_):
        xx, cc = line_back(r)
        return pltpu.make_async_remote_copy(buf.at[my_line], buf.at[my_line], ss.at[r], rs_.at[r],
                                            device_id=dev(z, y, xx, cc), device_id_type=MESH)

    far_first = [10, 9, 11, 6, 14, 2, 8, 5, 7, 13, 15, 1, 3, 4, 12]
    rows1 = [plane_copy(rowbuf, r, rs, rr) for r in far_first]
    cols1 = [line_copy(colbuf, r, cs, cr) for r in (5, 4, 3, 7, 2, 6, 1)]
    for cp in rows1 + cols1:
        cp.start()
    for cp in cols1 + rows1:
        cp.wait_recv()
    rb = rowbuf[...].reshape(16, 128)
    rb_l = pltpu.roll(rb, 64, 1)
    m = jnp.max(rb, axis=0, keepdims=True)
    lse_row = m + jnp.log(jnp.sum(rb_l * jnp.exp(rb - m), axis=0, keepdims=True))
    row_total = jnp.sum(jnp.where(lane1 < 64, lse_row, 0.0), axis=1, keepdims=True)
    cb = colbuf[...].reshape(8, 128)
    cb_l = pltpu.roll(cb, 96, 1)
    mc = jnp.max(cb, axis=0, keepdims=True)
    lse_col = mc + jnp.log(jnp.sum(cb_l * jnp.exp(cb - mc), axis=0, keepdims=True))
    col_total = jnp.sum(jnp.where(lane1 < 32, lse_col, 0.0), axis=1, keepdims=True)
    pos_sum = jnp.sum(jnp.sum(jnp.where(lane1 == 64, cb, 0.0), axis=0, keepdims=True), axis=1, keepdims=True)
    row2[my_slot] = jnp.broadcast_to(col_total - 2.0 * pos_sum, (1, 128))
    col2[my_line] = jnp.broadcast_to(row_total, (1, 128))
    rows2 = [plane_copy(row2, r, rs2, rr2) for r in far_first]
    cols2 = [line_copy(col2, r, cs2, cr2) for r in (5, 4, 3, 7, 2, 6, 1)]
    for cp in rows2 + cols2:
        cp.start()
    src = lax.broadcasted_iota(jnp.int32, (128, 128), 0)
    dst = lax.broadcasted_iota(jnp.int32, (128, 128), 1)

    def to_front(v, start):
        return pltpu.roll(v, lax.rem(128 - start, 128), 1)

    pos_front = to_front(pos_q, my_slot * 4)
    lq_ref[...] = to_front(lse_row, my_slot * 4) - pos_front
    ld_ref[...] = to_front(lse_col, my_line * 4) - pos_front
    for cp in cols2 + rows2:
        cp.wait_recv()
    total = (jnp.sum(row2[...].reshape(16, 128), axis=0, keepdims=True)
             + jnp.sum(col2[...].reshape(8, 128), axis=0, keepdims=True))
    lm_ref[...] = total / 1024.0

    for r in q_order:
        q_copy(r).wait_send()
    for cp in sends + rows1 + cols1 + rows2 + cols2:
        cp.wait_send()


def solution(mesh):
    batch_spec = P(('replica', 'data'))

    def local_loss(q_hidden, d_hidden, w_proj, q_mask, d_mask, temperature):
        any_spec = pl.BlockSpec(memory_space=pl.ANY)
        vmem = pl.BlockSpec(memory_space=pltpu.VMEM)
        dma = pltpu.SemaphoreType.DMA
        out = jax.ShapeDtypeStruct((1, 128), F32)
        lq, ld, lm = pl.pallas_call(
            kernel,
            out_shape=(out, out, out),
            in_specs=[any_spec] * 5 + [pl.BlockSpec(memory_space=pltpu.SMEM)],
            out_specs=(vmem, vmem, vmem),
            scratch_shapes=[
                pltpu.VMEM((4, 32, 768), BF16),
                pltpu.VMEM((4, 180, 768), BF16),
                pltpu.VMEM((768, 128), BF16),
                pltpu.VMEM((4, 32), jnp.int32),
                pltpu.VMEM((4, 180), jnp.int32),
                pltpu.VMEM((16, 128, 128), BF16),
                pltpu.VMEM((4, 2, 2, 2 * DPAD, 128), BF16),
                pltpu.VMEM((32, 2048), F32),
                pltpu.VMEM((16, 1, 128), F32),
                pltpu.VMEM((8, 1, 128), F32),
                pltpu.VMEM((16, 1, 128), F32),
                pltpu.VMEM((8, 1, 128), F32),
                dma((8,)), dma((16,)), dma((16,)), dma((6,)), dma((6,)), dma((8,)), dma((8,)),
                dma((16,)), dma((16,)), dma((8,)), dma((8,)), dma((16,)), dma((16,)), dma((8,)), dma((8,)),
            ],
            compiler_params=pltpu.CompilerParams(collective_id=0, has_side_effects=True,
                                                 vmem_limit_bytes=48 * 1024 * 1024),
        )(q_hidden, d_hidden, w_proj, q_mask, d_mask, temperature.reshape(1))
        return lq[0, :4], ld[0, :4], lm[0, :1]

    return jax.shard_map(local_loss, mesh=mesh, in_specs=(batch_spec, batch_spec, P(), batch_spec, batch_spec, P()),
                         out_specs=(batch_spec, batch_spec, P('replica')), check_vma=False)
```

```python
import jax
import jax.numpy as jnp
from jax import lax
from jax.experimental import pallas as pl
from jax.experimental.pallas import tpu as pltpu
from jax.sharding import PartitionSpec as P

F32 = jnp.float32
BF16 = jnp.bfloat16
MESH = pl.DeviceIdType.MESH
DPAD = 184
Q_ORDER = (0, 1, 3, 4, 12, 5, 7, 13, 15, 2, 8, 6, 14, 9, 11, 10)
OWN, LEFT, RIGHT, OPP = 0, 1, 2, 3


def unit_rows(raw):
    return raw / jnp.sqrt(jnp.sum(raw * raw, axis=-1, keepdims=True))


def iota(shape, axis):
    return lax.broadcasted_iota(jnp.int32, shape, axis)


def kernel(qh, dh, w, qm, dm, temp_ref, lq_ref, ld_ref, lm_ref,
           qbuf, dbuf, best, pick, rowbuf, colbuf, row2, col2,
           qs, qr, ds_, dr, ps, pr, rs, rr, cs, cr, rs2, rr2, cs2, cr2):
    me = lax.axis_index('data')
    c = lax.rem(me, 2)
    x = lax.rem(me // 2, 4)
    y = lax.rem(me // 8, 4)
    z = me // 32

    def dev(z_, y_, x_, c_):
        return {'data': ((z_ * 4 + y_) * 4 + x_) * 2 + c_}

    def plane(r):
        return lax.rem(z + r // 4, 4), lax.rem(y + r % 4, 4)

    def plane_back(r):
        return lax.rem(z + 4 - r // 4, 4), lax.rem(y + 4 - r % 4, 4)

    def line_back(r):
        return lax.rem(x + 4 - r // 2, 4), lax.rem(c + r % 2, 2)

    barrier = pltpu.get_barrier_semaphore()
    for r in Q_ORDER[1:]:
        zz, yy = plane_back(r)
        pl.semaphore_signal(barrier, inc=1, device_id=dev(zz, yy, x, c), device_id_type=MESH)
    for r in range(1, 8):
        xx, cc = line_back(r)
        pl.semaphore_signal(barrier, inc=1, device_id=dev(z, y, xx, cc), device_id_type=MESH)

    q_raw = jnp.dot(qh[...].reshape(128, 768), w[...], preferred_element_type=F32)
    q_col = jnp.transpose(jnp.concatenate([qm[...].astype(F32), jnp.zeros((4, 32), F32)], axis=0))
    q_valid = jnp.concatenate([q_col[:, i:i + 1] for i in range(4)], axis=0)
    qbuf[0] = jnp.where(q_valid == 1.0, unit_rows(q_raw), 0.0).astype(BF16)

    d_col = jnp.transpose(jnp.concatenate([dm[...].astype(F32), jnp.zeros((4, 180), F32)], axis=0))
    pos = iota((180, 1), 0)
    for h in range(2):
        parts = []
        for j in (2 * h, 2 * h + 1):
            u = unit_rows(jnp.dot(dh[j], w[...], preferred_element_type=F32))
            valid = d_col[:, j:j + 1] == 1.0
            first = jnp.min(jnp.where(valid, pos, 1000), axis=0, keepdims=True)
            vec = jnp.sum(jnp.where(pos == first, u, 0.0), axis=0, keepdims=True)
            parts += [jnp.where(valid, u, vec), jnp.broadcast_to(vec, (DPAD - 180, 128))]
        dbuf[OWN, 0, h] = jnp.concatenate(parts, axis=0).astype(BF16)

    def plane_slot(r):
        zz, yy = plane(r)
        return zz * 4 + yy

    tok = iota((128, 128), 0) // 32
    lanes = iota((128, 128), 1)
    for p in range(16):
        pick[p * 128:(p + 1) * 128, :] = (tok + 4 * plane_slot(Q_ORDER[p]) == lanes).astype(F32).astype(BF16)

    pl.semaphore_wait(barrier, 22)

    xr, xl = lax.rem(x + 1, 4), lax.rem(x + 3, 4)
    right, left, partner = dev(z, y, xr, c), dev(z, y, xl, c), dev(z, y, x, 1 - c)
    sends = []

    def rdma(src, dst, ssem, rsem, to):
        return pltpu.make_async_remote_copy(src, dst, ssem, rsem, device_id=to, device_id_type=MESH)

    def send(cp):
        cp.start()
        sends.append(cp)

    ICI = [(LEFT, 0), (LEFT, 1), (RIGHT, 0), (RIGHT, 1), (OPP, 0), (OPP, 1)]

    def to_right(src, h, i):
        return rdma(dbuf.at[src, 0, h], dbuf.at[ICI[i][0], 0, h], ds_.at[i], dr.at[i], right)

    def to_left(src, h, i):
        return rdma(dbuf.at[src, 0, h], dbuf.at[ICI[i][0], 0, h], ds_.at[i], dr.at[i], left)

    def to_partner(src, h):
        return rdma(dbuf.at[src, 0, h], dbuf.at[src, 1, h], ps.at[2 * src + h], pr.at[2 * src + h], partner)

    def q_copy(p):
        zz, yy = plane_back(Q_ORDER[p])
        return rdma(qbuf.at[0], qbuf.at[p], qs.at[p], qr.at[p], dev(zz, yy, x, c))

    for h in range(2):
        send(to_right(OWN, h, h))
        send(to_left(OWN, h, 2 + h))
        send(to_partner(OWN, h))
    for p in range(1, 16):
        send(q_copy(p))

    def wait_ici(i):
        side, h = ICI[i]
        to_right(OWN, h, i).wait_recv()
        if i == 0:
            send(to_right(LEFT, 0, 4))
        if i == 3:
            send(to_left(RIGHT, 1, 5))
        send(to_partner(side, h))

    def wait_partner(side, h):
        to_partner(side, h).wait_recv()

    def wait_q(k):
        for p in range(max(1, 4 * k), 4 * k + 4):
            q_copy(p).wait_recv()

    def block(pieces, chunks):
        n = len(pieces)
        lhs = jnp.concatenate([dbuf[piece] for piece in pieces], axis=0)
        for k in chunks:
            rhs = qbuf[4 * k:4 * k + 4].reshape(512, 128)
            sim = lax.dot_general(lhs, rhs, (((1,), (1,)), ((), ())), preferred_element_type=F32)
            top = jnp.max(sim.reshape(2 * n, DPAD, 512), axis=1)
            for i, (side, core, h) in enumerate(pieces):
                row = side * 8 + core * 4 + h * 2
                best[row:row + 2, k * 512:(k + 1) * 512] = top[2 * i:2 * i + 2]

    own = [(OWN, a, h) for a in range(2) for h in range(2)]
    near0 = [(s, a, 0) for s in (LEFT, RIGHT) for a in range(2)]
    near1 = [(s, a, 1) for s in (LEFT, RIGHT) for a in range(2)]
    opp = [(OPP, a, h) for a in range(2) for h in range(2)]

    wait_partner(OWN, 0)
    wait_partner(OWN, 1)
    wait_q(0)
    block(own, [0])
    wait_ici(0)
    wait_ici(2)
    wait_q(1)
    block(own, [1])
    wait_ici(1)
    wait_ici(3)
    wait_partner(LEFT, 0)
    wait_partner(RIGHT, 0)
    wait_q(2)
    block(own, [2])
    block(near0, [0, 1, 2])
    wait_ici(4)
    wait_ici(5)
    wait_partner(LEFT, 1)
    wait_partner(RIGHT, 1)
    block(near1, [0, 1, 2])
    wait_q(3)
    block(own, [3])
    block(near0, [3])
    block(near1, [3])
    wait_partner(OPP, 0)
    wait_partner(OPP, 1)
    block(opp, [0, 1, 2, 3])

    b = best[...]
    hi = b.astype(BF16)
    rest = b - hi.astype(F32)
    mid = rest.astype(BF16)
    low = (rest - mid.astype(F32)).astype(BF16)
    sums = jnp.dot(jnp.concatenate([hi, mid, low], axis=0), pick[...], preferred_element_type=F32)
    logits = ((sums[0:32] + sums[32:64]) + sums[64:96]) / temp_ref[0]
    lane = iota((32, 128), 1)
    sub = iota((32, 128), 0)
    lane1 = iota((1, 128), 1)
    my_slot = z * 4 + y
    my_line = x * 2 + c
    mine = (sub < 4) & (lane - my_slot * 4 == sub)
    pos_q = jnp.sum(jnp.where(mine, logits, 0.0), axis=0, keepdims=True)
    pos_total = jnp.sum(pos_q, axis=1, keepdims=True)
    m_row = jnp.max(logits, axis=0, keepdims=True)
    l_row = jnp.sum(jnp.exp(logits - m_row), axis=0, keepdims=True)
    qlane = lane < 64
    m_col = jnp.max(jnp.where(qlane, logits, -jnp.inf), axis=1, keepdims=True)
    l_col = jnp.sum(jnp.where(qlane, jnp.exp(logits - m_col), 0.0), axis=1, keepdims=True)
    side = sub // 8
    off = jnp.where(side == LEFT, 3, jnp.where(side == RIGHT, 1, jnp.where(side == OPP, 2, 0)))
    doc = ((x + off) & 3) * 8 + ((c + sub // 4) & 1) * 4 + (sub & 3)
    m_colr = jnp.sum(jnp.where(doc == lane, m_col, 0.0), axis=0, keepdims=True)
    l_colr = jnp.sum(jnp.where(doc == lane - 32, l_col, 0.0), axis=0, keepdims=True)
    rowbuf[my_slot] = jnp.where(lane1 < 64, m_row, pltpu.roll(l_row, 64, 1))
    colbuf[my_line] = jnp.where(lane1 == 64, pos_total, m_colr + l_colr)

    def plane_copy(buf, r, ss, rs_):
        zz, yy = plane_back(r)
        return rdma(buf.at[my_slot], buf.at[my_slot], ss.at[r], rs_.at[r], dev(zz, yy, x, c))

    def line_copy(buf, r, ss, rs_):
        xx, cc = line_back(r)
        return rdma(buf.at[my_line], buf.at[my_line], ss.at[r], rs_.at[r], dev(z, y, xx, cc))

    far_first = Q_ORDER[:0:-1]
    rows1 = [plane_copy(rowbuf, r, rs, rr) for r in far_first]
    cols1 = [line_copy(colbuf, r, cs, cr) for r in (5, 4, 3, 7, 2, 6, 1)]
    for cp in rows1 + cols1:
        cp.start()
    for cp in cols1 + rows1:
        cp.wait_recv()
    rb = rowbuf[...].reshape(16, 128)
    rb_l = pltpu.roll(rb, 64, 1)
    m = jnp.max(rb, axis=0, keepdims=True)
    lse_row = m + jnp.log(jnp.sum(rb_l * jnp.exp(rb - m), axis=0, keepdims=True))
    row_total = jnp.sum(jnp.where(lane1 < 64, lse_row, 0.0), axis=1, keepdims=True)
    cb = colbuf[...].reshape(8, 128)
    cb_l = pltpu.roll(cb, 96, 1)
    mc = jnp.max(cb, axis=0, keepdims=True)
    lse_col = mc + jnp.log(jnp.sum(cb_l * jnp.exp(cb - mc), axis=0, keepdims=True))
    col_total = jnp.sum(jnp.where(lane1 < 32, lse_col, 0.0), axis=1, keepdims=True)
    pos_sum = jnp.sum(jnp.sum(jnp.where(lane1 == 64, cb, 0.0), axis=0, keepdims=True), axis=1, keepdims=True)
    row2[my_slot] = jnp.broadcast_to(col_total - 2.0 * pos_sum, (1, 128))
    col2[my_line] = jnp.broadcast_to(row_total, (1, 128))
    rows2 = [plane_copy(row2, r, rs2, rr2) for r in far_first]
    cols2 = [line_copy(col2, r, cs2, cr2) for r in (5, 4, 3, 7, 2, 6, 1)]
    for cp in rows2 + cols2:
        cp.start()

    def to_front(v, start):
        return pltpu.roll(v, lax.rem(128 - start, 128), 1)

    pos_front = to_front(pos_q, my_slot * 4)
    lq_ref[...] = (to_front(lse_row, my_slot * 4) - pos_front)[0, :4]
    ld_ref[...] = (to_front(lse_col, my_line * 4) - pos_front)[0, :4]
    for cp in sends + rows1 + cols1:
        cp.wait_send()
    for cp in cols2 + rows2:
        cp.wait_recv()
    total = (jnp.sum(row2[...].reshape(16, 128), axis=0, keepdims=True)
             + jnp.sum(col2[...].reshape(8, 128), axis=0, keepdims=True))
    lm_ref[...] = (total / 1024.0)[0, :1]
    for cp in rows2 + cols2:
        cp.wait_send()


def solution(mesh):
    batch_spec = P(('replica', 'data'))

    def local_loss(q_hidden, d_hidden, w_proj, q_mask, d_mask, temperature):
        vmem = pl.BlockSpec(memory_space=pltpu.VMEM)
        dma = pltpu.SemaphoreType.DMA
        return pl.pallas_call(
            kernel,
            out_shape=tuple(jax.ShapeDtypeStruct((n,), F32) for n in (4, 4, 1)),
            in_specs=[vmem] * 5 + [pl.BlockSpec(memory_space=pltpu.SMEM)],
            out_specs=(vmem, vmem, vmem),
            scratch_shapes=[
                pltpu.VMEM((16, 128, 128), BF16),
                pltpu.VMEM((4, 2, 2, 2 * DPAD, 128), BF16),
                pltpu.VMEM((32, 2048), F32),
                pltpu.VMEM((2048, 128), BF16),
                pltpu.VMEM((16, 1, 128), F32),
                pltpu.VMEM((8, 1, 128), F32),
                pltpu.VMEM((16, 1, 128), F32),
                pltpu.VMEM((8, 1, 128), F32),
                dma((16,)), dma((16,)), dma((6,)), dma((6,)), dma((8,)), dma((8,)),
                dma((16,)), dma((16,)), dma((8,)), dma((8,)), dma((16,)), dma((16,)), dma((8,)), dma((8,)),
            ],
            compiler_params=pltpu.CompilerParams(collective_id=0, has_side_effects=True,
                                                 vmem_limit_bytes=48 * 1024 * 1024),
        )(q_hidden, d_hidden, w_proj, q_mask, d_mask, temperature.reshape(1))

    return jax.shard_map(local_loss, mesh=mesh, in_specs=(batch_spec, batch_spec, P(), batch_spec, batch_spec, P()),
                         out_specs=(batch_spec, batch_spec, P('replica')), check_vma=False)
```

```python
import jax
import jax.numpy as jnp
from jax import lax
from jax.experimental import pallas as pl
from jax.experimental.pallas import tpu as pltpu
from jax.sharding import PartitionSpec as P

F32 = jnp.float32
BF16 = jnp.bfloat16
MESH = pl.DeviceIdType.MESH
DPAD = 184
Q_ORDER = (0, 1, 3, 4, 12, 2, 8, 5, 7, 13, 15, 6, 14, 9, 11, 10)
P_Y2, P_Z2, P_FAR = 5, 6, 11
OWN, LEFT, RIGHT, OPP = 0, 1, 2, 3


def unit_rows(raw):
    return raw / jnp.sqrt(jnp.sum(raw * raw, axis=-1, keepdims=True))


def iota(shape, axis):
    return lax.broadcasted_iota(jnp.int32, shape, axis)


def kernel(qh, dh, w, qm, dm, temp_ref, lq_ref, ld_ref, lm_ref,
           qbuf, dbuf, best, pick, part, qs, qr, ds_, dr, ps, pr, fs, fr, ready):
    me = lax.axis_index('data')
    c = lax.rem(me, 2)
    x = lax.rem(me // 2, 4)
    y = lax.rem(me // 8, 4)
    z = me // 32

    def dev(z_, y_, x_, c_):
        return {'data': ((z_ * 4 + y_) * 4 + x_) * 2 + c_}

    def plane(r):
        return lax.rem(z + r // 4, 4), lax.rem(y + r % 4, 4)

    def plane_back(r):
        return lax.rem(z + 4 - r // 4, 4), lax.rem(y + 4 - r % 4, 4)

    def line_back(r):
        return lax.rem(x + 4 - r // 2, 4), lax.rem(c + r % 2, 2)

    barrier = pltpu.get_barrier_semaphore()
    for r in Q_ORDER[1:P_FAR]:
        zz, yy = plane_back(r)
        pl.semaphore_signal(barrier, inc=1, device_id=dev(zz, yy, x, c), device_id_type=MESH)
    for r in range(1, 8):
        xx, cc = line_back(r)
        pl.semaphore_signal(barrier, inc=1, device_id=dev(z, y, xx, cc), device_id_type=MESH)

    q_raw = jnp.dot(qh[...].reshape(128, 768), w[...], preferred_element_type=F32)
    q_col = jnp.transpose(jnp.concatenate([qm[...].astype(F32), jnp.zeros((4, 32), F32)], axis=0))
    q_valid = jnp.concatenate([q_col[:, i:i + 1] for i in range(4)], axis=0)
    qbuf[0] = jnp.where(q_valid == 1.0, unit_rows(q_raw), 0.0).astype(BF16)

    d_col = jnp.transpose(jnp.concatenate([dm[...].astype(F32), jnp.zeros((4, 180), F32)], axis=0))
    pos = iota((180, 1), 0)
    for h in range(2):
        parts = []
        for j in (2 * h, 2 * h + 1):
            u = unit_rows(jnp.dot(dh[j], w[...], preferred_element_type=F32))
            valid = d_col[:, j:j + 1] == 1.0
            first = jnp.min(jnp.where(valid, pos, 1000), axis=0, keepdims=True)
            vec = jnp.sum(jnp.where(pos == first, u, 0.0), axis=0, keepdims=True)
            parts += [jnp.where(valid, u, vec), jnp.broadcast_to(vec, (DPAD - 180, 128))]
        dbuf[OWN, 0, h] = jnp.concatenate(parts, axis=0).astype(BF16)

    pl.semaphore_wait(barrier, 17)

    xr, xl = lax.rem(x + 1, 4), lax.rem(x + 3, 4)
    right, left, partner = dev(z, y, xr, c), dev(z, y, xl, c), dev(z, y, x, 1 - c)
    sends = []

    def rdma(src, dst, ssem, rsem, to):
        return pltpu.make_async_remote_copy(src, dst, ssem, rsem, device_id=to, device_id_type=MESH)

    def send(cp):
        cp.start()
        sends.append(cp)

    ICI = [(LEFT, 0), (RIGHT, 1), (LEFT, 1), (RIGHT, 0), (OPP, 0), (OPP, 1)]

    def to_right(src, h, i):
        return rdma(dbuf.at[src, 0, h], dbuf.at[ICI[i][0], 0, h], ds_.at[i], dr.at[i], right)

    def to_left(src, h, i):
        return rdma(dbuf.at[src, 0, h], dbuf.at[ICI[i][0], 0, h], ds_.at[i], dr.at[i], left)

    def to_partner(src, h):
        return rdma(dbuf.at[src, 0, h], dbuf.at[src, 1, h], ps.at[2 * src + h], pr.at[2 * src + h], partner)

    def q_copy(p):
        dz, dy = Q_ORDER[p] // 4, Q_ORDER[p] % 4
        src = 0
        if p >= P_FAR:
            if dy == 2:
                src, dy = P_Y2, 0
            else:
                src, dz = P_Z2, 0
        zz, yy = plane_back(4 * dz + dy)
        return rdma(qbuf.at[src], qbuf.at[p], qs.at[p], qr.at[p], dev(zz, yy, x, c))

    send(to_right(OWN, 0, 0))
    send(to_left(OWN, 1, 1))
    for p in (P_Y2, P_Z2, 1, 2, 3, 4):
        send(q_copy(p))
    send(to_partner(OWN, 0))
    send(to_partner(OWN, 1))
    send(to_right(OWN, 1, 2))
    send(to_left(OWN, 0, 3))
    for p in range(P_Z2 + 1, P_FAR):
        send(q_copy(p))

    def plane_slot(r):
        zz, yy = plane(r)
        return zz * 4 + yy

    tok = iota((128, 128), 0) // 32
    lanes = iota((128, 128), 1)
    for p in range(16):
        pick[p * 128:(p + 1) * 128, :] = (tok + 4 * plane_slot(Q_ORDER[p]) == lanes).astype(F32).astype(BF16)

    def wait_ici(i):
        side, h = ICI[i]
        to_right(OWN, h, i).wait_recv()
        if i == 0:
            send(to_right(LEFT, 0, 4))
        if i == 1:
            send(to_left(RIGHT, 1, 5))
        send(to_partner(side, h))

    def wait_partner(side, h):
        to_partner(side, h).wait_recv()

    def wait_q(*blocks):
        for p in blocks:
            q_copy(p).wait_recv()

    def block(pieces, chunks):
        n = len(pieces)
        lhs = jnp.concatenate([dbuf[piece] for piece in pieces], axis=0)
        for k in chunks:
            rhs = qbuf[4 * k:4 * k + 4].reshape(512, 128)
            sim = lax.dot_general(lhs, rhs, (((1,), (1,)), ((), ())), preferred_element_type=F32)
            top = jnp.max(sim.reshape(2 * n, DPAD, 512), axis=1)
            for i, (side, core, h) in enumerate(pieces):
                row = side * 8 + core * 4 + h * 2
                best[row:row + 2, k * 512:(k + 1) * 512] = top[2 * i:2 * i + 2]

    def group(side, h):
        return [(side, a, h) for a in range(2)]

    own = group(OWN, 0) + group(OWN, 1)
    near0 = group(LEFT, 0) + group(RIGHT, 1)
    near1 = group(LEFT, 1) + group(RIGHT, 0)

    wait_partner(OWN, 0)
    wait_partner(OWN, 1)
    wait_q(1, 2, 3)
    block(own, [0])
    wait_q(P_Y2, P_Z2)
    for p in range(P_FAR, 16):
        send(q_copy(p))
    wait_ici(0)
    wait_ici(1)
    wait_q(4, 7)
    block(own, [1])
    wait_ici(2)
    wait_ici(3)
    wait_partner(LEFT, 0)
    wait_partner(RIGHT, 1)
    block(near0, [0, 1])
    wait_q(8, 9, 10, 11)
    block(own, [2])
    block(near0, [2])
    wait_partner(LEFT, 1)
    wait_partner(RIGHT, 0)
    wait_ici(4)
    wait_ici(5)
    wait_q(12, 13, 14, 15)
    for r in range(1, 16):
        zz, yy = plane_back(r)
        pl.semaphore_signal(ready, inc=1, device_id=dev(zz, yy, x, c), device_id_type=MESH)
    block(near1, [0, 1, 2])
    block(own, [3])
    block(near0, [3])
    block(near1, [3])
    block([(OPP, 0, 0), (OPP, 0, 1)], [0, 1, 2, 3])
    wait_partner(OPP, 0)
    wait_partner(OPP, 1)
    block([(OPP, 1, 0), (OPP, 1, 1)], [0, 1, 2, 3])

    b = best[...]
    hi = b.astype(BF16)
    rest = b - hi.astype(F32)
    mid = rest.astype(BF16)
    low = (rest - mid.astype(F32)).astype(BF16)
    sums = jnp.dot(jnp.concatenate([hi, mid, low], axis=0), pick[...], preferred_element_type=F32)
    logits = ((sums[0:32] + sums[32:64]) + sums[64:96]) / temp_ref[0]
    lane = iota((32, 128), 1)
    sub = iota((32, 128), 0)
    lane1 = iota((1, 128), 1)
    my_slot = z * 4 + y
    my_line = x * 2 + c
    mine = (sub < 4) & (lane - my_slot * 4 == sub)
    pos_q = jnp.sum(jnp.where(mine, logits, 0.0), axis=0, keepdims=True)
    pos_total = jnp.sum(pos_q, axis=1, keepdims=True)
    m_row = jnp.max(logits, axis=0, keepdims=True)
    l_row = jnp.sum(jnp.exp(logits - m_row), axis=0, keepdims=True)
    qlane = lane < 64
    m_col = jnp.max(jnp.where(qlane, logits, -jnp.inf), axis=1, keepdims=True)
    l_col = jnp.sum(jnp.where(qlane, jnp.exp(logits - m_col), 0.0), axis=1, keepdims=True)
    side = sub // 8
    off = jnp.where(side == LEFT, 3, jnp.where(side == RIGHT, 1, jnp.where(side == OPP, 2, 0)))
    doc = ((x + off) & 3) * 8 + ((c + sub // 4) & 1) * 4 + (sub & 3)
    m_colr = jnp.sum(jnp.where(doc == lane - 64, m_col, 0.0), axis=0, keepdims=True)
    l_colr = jnp.sum(jnp.where(doc == lane - 64, l_col, 0.0), axis=0, keepdims=True)
    top_row = jnp.where(lane1 < 64, m_row, jnp.where(lane1 == 96, pos_total, m_colr))
    sum_row = jnp.where(lane1 < 64, l_row, l_colr)
    part[me] = jnp.concatenate([top_row, sum_row], axis=0)
    pl.semaphore_wait(ready, 15)

    def hops(r):
        return sum((0, 1, 2, 1)[(r >> b) & 3] for b in (1, 3, 5))

    for r in sorted(range(1, 128), key=hops, reverse=True):
        rdma(part.at[me], part.at[me], fs, fr, {'data': me ^ r}).start()
    for cp in sends:
        cp.wait_send()
    everyone = rdma(part.at[0:127], part.at[0:127], fs, fr, partner)
    everyone.wait_recv()
    tops = part[:, 0, :].reshape(16, 8, 128)
    adds = part[:, 1, :].reshape(16, 8, 128)
    mr = jnp.max(tops, axis=0)
    lse_row = mr + jnp.log(jnp.sum(adds * jnp.exp(tops - mr[None]), axis=0))
    mc = jnp.max(tops, axis=1, keepdims=True)
    lse_col = (mc + jnp.log(jnp.sum(adds * jnp.exp(tops - mc), axis=1, keepdims=True))).reshape(16, 128)
    lane8 = iota((8, 128), 1)
    lane16 = iota((16, 128), 1)
    row_sum = jnp.sum(jnp.where(lane8 < 64, lse_row, 0.0), axis=0, keepdims=True)
    col_sum = jnp.sum(jnp.where((lane16 >= 64) & (lane16 < 96), lse_col, 0.0), axis=0, keepdims=True)
    pos_sum = jnp.sum(jnp.sum(tops, axis=0), axis=0, keepdims=True)
    total = jnp.sum(row_sum + col_sum - jnp.where(lane1 == 96, 2.0 * pos_sum, 0.0), axis=1, keepdims=True)
    lm_ref[...] = (total / 1024.0)[0, :1]

    def to_front(v, start):
        return pltpu.roll(v, lax.rem(128 - start, 128), 1)

    pos_front = to_front(pos_q, my_slot * 4)
    my_row = jnp.sum(jnp.where(iota((8, 128), 0) == my_line, lse_row, 0.0), axis=0, keepdims=True)
    my_col = jnp.sum(jnp.where(iota((16, 128), 0) == my_slot, lse_col, 0.0), axis=0, keepdims=True)
    lq_ref[...] = (to_front(my_row, my_slot * 4) - pos_front)[0, :4]
    ld_ref[...] = (to_front(my_col, 64 + my_line * 4) - pos_front)[0, :4]
    everyone.wait_send()


def solution(mesh):
    batch_spec = P(('replica', 'data'))

    def local_loss(q_hidden, d_hidden, w_proj, q_mask, d_mask, temperature):
        vmem = pl.BlockSpec(memory_space=pltpu.VMEM)
        dma = pltpu.SemaphoreType.DMA
        return pl.pallas_call(
            kernel,
            out_shape=tuple(jax.ShapeDtypeStruct((n,), F32) for n in (4, 4, 1)),
            in_specs=[vmem] * 5 + [pl.BlockSpec(memory_space=pltpu.SMEM)],
            out_specs=(vmem, vmem, vmem),
            scratch_shapes=[
                pltpu.VMEM((16, 128, 128), BF16),
                pltpu.VMEM((4, 2, 2, 2 * DPAD, 128), BF16),
                pltpu.VMEM((32, 2048), F32),
                pltpu.VMEM((2048, 128), BF16),
                pltpu.VMEM((128, 2, 128), F32),
                dma((16,)), dma((16,)), dma((6,)), dma((6,)), dma((8,)), dma((8,)), dma, dma,
                pltpu.SemaphoreType.REGULAR,
            ],
            compiler_params=pltpu.CompilerParams(collective_id=0, has_side_effects=True,
                                                 vmem_limit_bytes=48 * 1024 * 1024),
        )(q_hidden, d_hidden, w_proj, q_mask, d_mask, temperature.reshape(1))

    return jax.shard_map(local_loss, mesh=mesh, in_specs=(batch_spec, batch_spec, P(), batch_spec, batch_spec, P()),
                         out_specs=(batch_spec, batch_spec, P('replica')), check_vma=False)
```

```python
import jax
import jax.numpy as jnp
from jax import lax
from jax.experimental import pallas as pl
from jax.experimental.pallas import tpu as pltpu
from jax.sharding import PartitionSpec as P

F32 = jnp.float32
BF16 = jnp.bfloat16
MESH = pl.DeviceIdType.MESH
DPAD = 184
Q_ORDER = (0, 1, 3, 4, 12, 2, 8, 5, 7, 13, 15, 6, 14, 9, 11, 10)
P_Y2, P_Z2, P_FAR = 5, 6, 11
OWN, LEFT, RIGHT, OPP = 0, 1, 2, 3


def unit_rows(raw):
    return raw / jnp.sqrt(jnp.sum(raw * raw, axis=-1, keepdims=True))


def iota(shape, axis):
    return lax.broadcasted_iota(jnp.int32, shape, axis)


def kernel(qh, dh, w, qm, dm, temp_ref, lq_ref, ld_ref, lm_ref,
           qbuf, dbuf, best, pick, part, qs, qr, ds_, dr, ps, pr, fs, fr, ready):
    me = lax.axis_index('data')
    c = lax.rem(me, 2)
    x = lax.rem(me // 2, 4)
    y = lax.rem(me // 8, 4)
    z = me // 32

    def dev(z_, y_, x_, c_):
        return {'data': ((z_ * 4 + y_) * 4 + x_) * 2 + c_}

    def plane(r):
        return lax.rem(z + r // 4, 4), lax.rem(y + r % 4, 4)

    def plane_back(r):
        return lax.rem(z + 4 - r // 4, 4), lax.rem(y + 4 - r % 4, 4)

    def line_back(r):
        return lax.rem(x + 4 - r // 2, 4), lax.rem(c + r % 2, 2)

    barrier = pltpu.get_barrier_semaphore()
    for r in Q_ORDER[1:P_FAR]:
        zz, yy = plane_back(r)
        pl.semaphore_signal(barrier, inc=1, device_id=dev(zz, yy, x, c), device_id_type=MESH)
    for r in range(1, 8):
        xx, cc = line_back(r)
        pl.semaphore_signal(barrier, inc=1, device_id=dev(z, y, xx, cc), device_id_type=MESH)

    q_raw = jnp.dot(qh[...].reshape(128, 768), w[...], preferred_element_type=F32)
    q_col = jnp.transpose(jnp.concatenate([qm[...].astype(F32), jnp.zeros((4, 32), F32)], axis=0))
    q_valid = jnp.concatenate([q_col[:, i:i + 1] for i in range(4)], axis=0)
    qbuf[0] = jnp.where(q_valid == 1.0, unit_rows(q_raw), 0.0).astype(BF16)

    d_col = jnp.transpose(jnp.concatenate([dm[...].astype(F32), jnp.zeros((4, 180), F32)], axis=0))
    pos = iota((180, 1), 0)
    for h in range(2):
        parts = []
        for j in (2 * h, 2 * h + 1):
            u = unit_rows(jnp.dot(dh[j], w[...], preferred_element_type=F32))
            valid = d_col[:, j:j + 1] == 1.0
            first = jnp.min(jnp.where(valid, pos, 1000), axis=0, keepdims=True)
            vec = jnp.sum(jnp.where(pos == first, u, 0.0), axis=0, keepdims=True)
            parts += [jnp.where(valid, u, vec), jnp.broadcast_to(vec, (DPAD - 180, 128))]
        dbuf[OWN, 0, h] = jnp.concatenate(parts, axis=0).astype(BF16)

    pl.semaphore_wait(barrier, 17)

    xr, xl = lax.rem(x + 1, 4), lax.rem(x + 3, 4)
    right, left, partner = dev(z, y, xr, c), dev(z, y, xl, c), dev(z, y, x, 1 - c)
    sends = []

    def rdma(src, dst, ssem, rsem, to):
        return pltpu.make_async_remote_copy(src, dst, ssem, rsem, device_id=to, device_id_type=MESH)

    def send(cp):
        cp.start()
        sends.append(cp)

    ICI = [(LEFT, 0), (RIGHT, 1), (LEFT, 1), (RIGHT, 0), (OPP, 0), (OPP, 1)]

    def to_right(src, h, i):
        return rdma(dbuf.at[src, 0, h], dbuf.at[ICI[i][0], 0, h], ds_.at[i], dr.at[i], right)

    def to_left(src, h, i):
        return rdma(dbuf.at[src, 0, h], dbuf.at[ICI[i][0], 0, h], ds_.at[i], dr.at[i], left)

    def to_partner(src, h):
        return rdma(dbuf.at[src, 0, h], dbuf.at[src, 1, h], ps.at[2 * src + h], pr.at[2 * src + h], partner)

    def q_copy(p):
        dz, dy = Q_ORDER[p] // 4, Q_ORDER[p] % 4
        src = 0
        if p >= P_FAR:
            if dy == 2:
                src, dy = P_Y2, 0
            else:
                src, dz = P_Z2, 0
        zz, yy = plane_back(4 * dz + dy)
        return rdma(qbuf.at[src], qbuf.at[p], qs.at[p], qr.at[p], dev(zz, yy, x, c))

    send(to_right(OWN, 0, 0))
    send(to_left(OWN, 1, 1))
    for p in (P_Y2, P_Z2, 1, 2, 3, 4):
        send(q_copy(p))
    send(to_partner(OWN, 0))
    send(to_partner(OWN, 1))
    send(to_right(OWN, 1, 2))
    send(to_left(OWN, 0, 3))
    for p in range(P_Z2 + 1, P_FAR):
        send(q_copy(p))

    def plane_slot(r):
        zz, yy = plane(r)
        return zz * 4 + yy

    tok = iota((128, 128), 0) // 32
    lanes = iota((128, 128), 1)
    for p in range(16):
        pick[p * 128:(p + 1) * 128, :] = (tok + 4 * plane_slot(Q_ORDER[p]) == lanes).astype(F32).astype(BF16)

    def wait_ici(i):
        side, h = ICI[i]
        to_right(OWN, h, i).wait_recv()
        if i == 0:
            send(to_right(LEFT, 0, 4))
        if i == 1:
            send(to_left(RIGHT, 1, 5))
        send(to_partner(side, h))

    def wait_partner(side, h):
        to_partner(side, h).wait_recv()

    def wait_q(*blocks):
        for p in blocks:
            q_copy(p).wait_recv()

    def block(pieces, chunks):
        n = len(pieces)
        lhs = jnp.concatenate([dbuf[piece] for piece in pieces], axis=0)
        for lo, hi in chunks:
            width = (hi - lo) * 128
            rhs = qbuf[lo:hi].reshape(width, 128)
            sim = lax.dot_general(lhs, rhs, (((1,), (1,)), ((), ())), preferred_element_type=F32)
            top = jnp.max(sim.reshape(2 * n, DPAD, width), axis=1)
            for i, (side, core, h) in enumerate(pieces):
                row = side * 8 + core * 4 + h * 2
                best[row:row + 2, lo * 128:hi * 128] = top[2 * i:2 * i + 2]

    def pair(core, *halves):
        return [(side, core, h) for side, h in halves]

    own = pair(0, (OWN, 0), (OWN, 1)) + pair(1, (OWN, 0), (OWN, 1))
    near0 = [pair(a, (LEFT, 0), (RIGHT, 1)) for a in range(2)]
    near1 = [pair(a, (LEFT, 1), (RIGHT, 0)) for a in range(2)]
    opp = [pair(a, (OPP, 0), (OPP, 1)) for a in range(2)]
    A, B, C, D = (0, 4), (4, 8), (8, 10), (10, 16)

    wait_partner(OWN, 0)
    wait_partner(OWN, 1)
    wait_q(1, 2, 3)
    block(own, [A])
    wait_q(P_Y2, P_Z2)
    for p in range(P_FAR, 16):
        send(q_copy(p))
    wait_ici(0)
    wait_ici(1)
    block(near0[0], [A])
    wait_q(4, 7)
    block(own, [B])
    block(near0[0], [B])
    wait_partner(LEFT, 0)
    wait_partner(RIGHT, 1)
    block(near0[1], [A, B])
    wait_ici(2)
    wait_ici(3)
    wait_q(8, 9)
    block(own + near0[0] + near0[1], [C])
    block(near1[0], [A, B, C])
    wait_partner(LEFT, 1)
    wait_partner(RIGHT, 0)
    block(near1[1], [A, B, C])
    wait_q(10, 11, 12, 13, 14, 15)
    for r in range(1, 16):
        zz, yy = plane_back(r)
        pl.semaphore_signal(ready, inc=1, device_id=dev(zz, yy, x, c), device_id_type=MESH)
    block(own, [D])
    wait_ici(4)
    wait_ici(5)
    block(near0[0] + near0[1] + near1[0] + near1[1], [D])
    block(opp[0], [A, B, C, D])
    wait_partner(OPP, 0)
    wait_partner(OPP, 1)
    block(opp[1], [A, B, C, D])

    b = best[...]
    hi = b.astype(BF16)
    rest = b - hi.astype(F32)
    mid = rest.astype(BF16)
    low = (rest - mid.astype(F32)).astype(BF16)
    sums = jnp.dot(jnp.concatenate([hi, mid, low], axis=0), pick[...], preferred_element_type=F32)
    logits = ((sums[0:32] + sums[32:64]) + sums[64:96]) / temp_ref[0]
    lane = iota((32, 128), 1)
    sub = iota((32, 128), 0)
    lane1 = iota((1, 128), 1)
    my_slot = z * 4 + y
    my_line = x * 2 + c
    mine = (sub < 4) & (lane - my_slot * 4 == sub)
    pos_q = jnp.sum(jnp.where(mine, logits, 0.0), axis=0, keepdims=True)
    pos_total = jnp.sum(pos_q, axis=1, keepdims=True)
    m_row = jnp.max(logits, axis=0, keepdims=True)
    l_row = jnp.sum(jnp.exp(logits - m_row), axis=0, keepdims=True)
    qlane = lane < 64
    m_col = jnp.max(jnp.where(qlane, logits, -jnp.inf), axis=1, keepdims=True)
    l_col = jnp.sum(jnp.where(qlane, jnp.exp(logits - m_col), 0.0), axis=1, keepdims=True)
    side = sub // 8
    off = jnp.where(side == LEFT, 3, jnp.where(side == RIGHT, 1, jnp.where(side == OPP, 2, 0)))
    doc = ((x + off) & 3) * 8 + ((c + sub // 4) & 1) * 4 + (sub & 3)
    m_colr = jnp.sum(jnp.where(doc == lane - 64, m_col, 0.0), axis=0, keepdims=True)
    l_colr = jnp.sum(jnp.where(doc == lane - 64, l_col, 0.0), axis=0, keepdims=True)
    top_row = jnp.where(lane1 < 64, m_row, jnp.where(lane1 == 96, pos_total, m_colr))
    sum_row = jnp.where(lane1 < 64, l_row, l_colr)
    part[me] = jnp.concatenate([top_row, sum_row], axis=0)
    pl.semaphore_wait(ready, 15)

    def hops(r):
        return sum((0, 1, 2, 1)[(r >> b) & 3] for b in (1, 3, 5))

    for r in sorted(range(1, 128), key=hops, reverse=True):
        rdma(part.at[me], part.at[me], fs, fr, {'data': me ^ r}).start()
    for cp in sends:
        cp.wait_send()
    everyone = rdma(part.at[0:127], part.at[0:127], fs, fr, partner)
    everyone.wait_recv()
    tops = part[:, 0, :].reshape(16, 8, 128)
    adds = part[:, 1, :].reshape(16, 8, 128)
    mr = jnp.max(tops, axis=0)
    lse_row = mr + jnp.log(jnp.sum(adds * jnp.exp(tops - mr[None]), axis=0))
    mc = jnp.max(tops, axis=1, keepdims=True)
    lse_col = (mc + jnp.log(jnp.sum(adds * jnp.exp(tops - mc), axis=1, keepdims=True))).reshape(16, 128)
    lane8 = iota((8, 128), 1)
    lane16 = iota((16, 128), 1)
    row_sum = jnp.sum(jnp.where(lane8 < 64, lse_row, 0.0), axis=0, keepdims=True)
    col_sum = jnp.sum(jnp.where((lane16 >= 64) & (lane16 < 96), lse_col, 0.0), axis=0, keepdims=True)
    pos_sum = jnp.sum(jnp.sum(tops, axis=0), axis=0, keepdims=True)
    total = jnp.sum(row_sum + col_sum - jnp.where(lane1 == 96, 2.0 * pos_sum, 0.0), axis=1, keepdims=True)
    lm_ref[...] = jnp.broadcast_to(total / 1024.0, (1, 128))

    def to_front(v, start):
        return pltpu.roll(v, lax.rem(128 - start, 128), 1)

    pos_front = to_front(pos_q, my_slot * 4)
    my_row = jnp.sum(jnp.where(iota((8, 128), 0) == my_line, lse_row, 0.0), axis=0, keepdims=True)
    my_col = jnp.sum(jnp.where(iota((16, 128), 0) == my_slot, lse_col, 0.0), axis=0, keepdims=True)
    lq_ref[...] = (to_front(my_row, my_slot * 4) - pos_front)
    ld_ref[...] = (to_front(my_col, 64 + my_line * 4) - pos_front)
    everyone.wait_send()


def solution(mesh):
    batch_spec = P(('replica', 'data'))

    def local_loss(q_hidden, d_hidden, w_proj, q_mask, d_mask, temperature):
        vmem = pl.BlockSpec(memory_space=pltpu.VMEM)
        dma = pltpu.SemaphoreType.DMA
        lq, ld, lm = pl.pallas_call(
            kernel,
            out_shape=(jax.ShapeDtypeStruct((1, 128), F32),) * 3,
            in_specs=[vmem] * 5 + [pl.BlockSpec(memory_space=pltpu.SMEM)],
            out_specs=(vmem, vmem, vmem),
            scratch_shapes=[
                pltpu.VMEM((16, 128, 128), BF16),
                pltpu.VMEM((4, 2, 2, 2 * DPAD, 128), BF16),
                pltpu.VMEM((32, 2048), F32),
                pltpu.VMEM((2048, 128), BF16),
                pltpu.VMEM((128, 2, 128), F32),
                dma((16,)), dma((16,)), dma((6,)), dma((6,)), dma((8,)), dma((8,)), dma, dma,
                pltpu.SemaphoreType.REGULAR,
            ],
            compiler_params=pltpu.CompilerParams(collective_id=0, has_side_effects=True,
                                                 vmem_limit_bytes=48 * 1024 * 1024),
        )(q_hidden, d_hidden, w_proj, q_mask, d_mask, temperature.reshape(1))
        return lq[0, :4], ld[0, :4], lm[0, :1]

    return jax.shard_map(local_loss, mesh=mesh, in_specs=(batch_spec, batch_spec, P(), batch_spec, batch_spec, P()),
                         out_specs=(batch_spec, batch_spec, P('replica')), check_vma=False)
```

```python
import jax
import jax.numpy as jnp
from jax import lax
from jax.experimental import pallas as pl
from jax.experimental.pallas import tpu as pltpu
from jax.sharding import PartitionSpec as P

F32 = jnp.float32
BF16 = jnp.bfloat16
MESH = pl.DeviceIdType.MESH
HALF = 368
CUTS = (0, 46, 92, 136, 180)
Q_ORDER = (0, 1, 3, 4, 12, 2, 8, 5, 7, 13, 15, 6, 14, 9, 11, 10)
P_Y2, P_Z2, P_FAR = 5, 6, 11
OWN, LEFT, RIGHT, OPP = 0, 1, 2, 3


def unit_rows(raw):
    return raw / jnp.sqrt(jnp.sum(raw * raw, axis=-1, keepdims=True))


def iota(shape, axis):
    return lax.broadcasted_iota(jnp.int32, shape, axis)


def kernel(q_hbm, d_hbm, w_hbm, qm_hbm, dm_hbm, temp_ref, lq_ref, ld_ref, lm_ref,
           qh, dh, w, qm, dm, lsem, live, qbuf, dbuf, best, pick, part, qs, qr, ds_, dr, ps, pr, fs, fr, ready):
    me = lax.axis_index('data')
    c = lax.rem(me, 2)
    x = lax.rem(me // 2, 4)
    y = lax.rem(me // 8, 4)
    z = me // 32

    def dev(z_, y_, x_, c_):
        return {'data': ((z_ * 4 + y_) * 4 + x_) * 2 + c_}

    def plane(r):
        return lax.rem(z + r // 4, 4), lax.rem(y + r % 4, 4)

    def plane_back(r):
        return lax.rem(z + 4 - r // 4, 4), lax.rem(y + 4 - r % 4, 4)

    def line_back(r):
        return lax.rem(x + 4 - r // 2, 4), lax.rem(c + r % 2, 2)

    loads = [pltpu.make_async_copy(dm_hbm, dm, lsem.at[0]), pltpu.make_async_copy(w_hbm, w, lsem.at[1])]
    for i in range(4):
        rows = pl.ds(CUTS[i], CUTS[i + 1] - CUTS[i])
        loads.append(pltpu.make_async_copy(d_hbm.at[rows], dh.at[rows], lsem.at[2 + i]))
    loads += [pltpu.make_async_copy(q_hbm, qh, lsem.at[6]), pltpu.make_async_copy(qm_hbm, qm, lsem.at[7])]
    for cp in loads:
        cp.start()

    barrier = pltpu.get_barrier_semaphore()
    for r in Q_ORDER[1:P_FAR]:
        zz, yy = plane_back(r)
        pl.semaphore_signal(barrier, inc=1, device_id=dev(zz, yy, x, c), device_id_type=MESH)
    for r in range(1, 8):
        xx, cc = line_back(r)
        pl.semaphore_signal(barrier, inc=1, device_id=dev(z, y, xx, cc), device_id_type=MESH)

    loads[0].wait()
    d_col = jnp.transpose(jnp.concatenate([dm[...].astype(F32), jnp.zeros((4, 180), F32)], axis=0))
    for j in range(4):
        live[pl.ds(j, 180, stride=4), :] = jnp.broadcast_to(d_col[:, j:j + 1], (180, 128))
    valid = live[...].reshape(90, 8, 128) == 1.0
    token = (iota((720, 128), 0) // 4).reshape(90, 8, 128)
    first = jnp.min(jnp.where(valid, token, 1000), axis=0)
    first = jnp.minimum(first, pltpu.roll(first, 4, 0))
    for cp in loads[1:]:
        cp.wait()

    halves = [dh[0:92].reshape(HALF, 768), dh[92:180].reshape(720 - HALF, 768)]
    u = jnp.concatenate([unit_rows(jnp.dot(rows, w[...], preferred_element_type=F32)) for rows in halves], axis=0)
    u = u.reshape(90, 8, 128)
    vec = jnp.sum(jnp.where(token == first[None], u, 0.0), axis=0)
    vec = vec + pltpu.roll(vec, 4, 0)
    dbuf[OWN, 0] = jnp.where(valid, u, vec[None]).reshape(720, 128).astype(BF16)

    q_raw = jnp.dot(qh[...].reshape(128, 768), w[...], preferred_element_type=F32)
    q_col = jnp.transpose(jnp.concatenate([qm[...].astype(F32), jnp.zeros((4, 32), F32)], axis=0))
    q_valid = jnp.concatenate([q_col[:, i:i + 1] for i in range(4)], axis=0)
    qbuf[0] = jnp.where(q_valid == 1.0, unit_rows(q_raw), 0.0).astype(BF16)

    pl.semaphore_wait(barrier, 17)

    xr, xl = lax.rem(x + 1, 4), lax.rem(x + 3, 4)
    right, left, partner = dev(z, y, xr, c), dev(z, y, xl, c), dev(z, y, x, 1 - c)
    sends = []

    def rdma(src, dst, ssem, rsem, to):
        return pltpu.make_async_remote_copy(src, dst, ssem, rsem, device_id=to, device_id_type=MESH)

    def send(cp):
        cp.start()
        sends.append(cp)

    ICI = [(LEFT, 0), (RIGHT, 1), (LEFT, 1), (RIGHT, 0), (OPP, 0), (OPP, 1)]

    SPAN = (pl.ds(0, HALF), pl.ds(HALF, 720 - HALF))

    def to_right(src, h, i):
        return rdma(dbuf.at[src, 0, SPAN[h]], dbuf.at[ICI[i][0], 0, SPAN[h]], ds_.at[i], dr.at[i], right)

    def to_left(src, h, i):
        return rdma(dbuf.at[src, 0, SPAN[h]], dbuf.at[ICI[i][0], 0, SPAN[h]], ds_.at[i], dr.at[i], left)

    def to_partner(src, h):
        return rdma(dbuf.at[src, 0, SPAN[h]], dbuf.at[src, 1, SPAN[h]], ps.at[2 * src + h], pr.at[2 * src + h], partner)

    def q_copy(p):
        dz, dy = Q_ORDER[p] // 4, Q_ORDER[p] % 4
        src = 0
        if p >= P_FAR:
            if dy == 2:
                src, dy = P_Y2, 0
            else:
                src, dz = P_Z2, 0
        zz, yy = plane_back(4 * dz + dy)
        return rdma(qbuf.at[src], qbuf.at[p], qs.at[p], qr.at[p], dev(zz, yy, x, c))

    send(to_right(OWN, 0, 0))
    send(to_left(OWN, 1, 1))
    for p in (P_Y2, P_Z2, 1, 2, 3, 4):
        send(q_copy(p))
    send(to_partner(OWN, 0))
    send(to_partner(OWN, 1))
    send(to_right(OWN, 1, 2))
    send(to_left(OWN, 0, 3))
    for p in range(P_Z2 + 1, P_FAR):
        send(q_copy(p))

    def plane_slot(r):
        zz, yy = plane(r)
        return zz * 4 + yy

    tok = iota((128, 128), 0) // 32
    lanes = iota((128, 128), 1)
    for p in range(16):
        pick[p * 128:(p + 1) * 128, :] = (tok + 4 * plane_slot(Q_ORDER[p]) == lanes).astype(F32).astype(BF16)

    def wait_ici(i):
        side, h = ICI[i]
        to_right(OWN, h, i).wait_recv()
        if i == 0:
            send(to_right(LEFT, 0, 4))
        if i == 1:
            send(to_left(RIGHT, 1, 5))
        send(to_partner(side, h))

    def wait_partner(side, h):
        to_partner(side, h).wait_recv()

    def wait_q(*blocks):
        for p in blocks:
            q_copy(p).wait_recv()

    def block(pieces, chunks):
        lhs = jnp.concatenate([dbuf[side, core, SPAN[h], :] for side, core, h in pieces], axis=0)
        for lo, hi in chunks:
            width = (hi - lo) * 128
            rhs = qbuf[lo:hi].reshape(width, 128)
            sim = lax.dot_general(lhs, rhs, (((1,), (1,)), ((), ())), preferred_element_type=F32)
            at = 0
            for side, core, h in pieces:
                rows = HALF if h == 0 else 720 - HALF
                top = jnp.max(sim[at:at + rows].reshape(rows // 8, 8, width), axis=0)
                best[side, core, h, :, lo * 128:hi * 128] = top
                at += rows

    def pair(core, *halves):
        return [(side, core, h) for side, h in halves]

    own = pair(0, (OWN, 0), (OWN, 1)) + pair(1, (OWN, 0), (OWN, 1))
    near0 = [pair(a, (LEFT, 0), (RIGHT, 1)) for a in range(2)]
    near1 = [pair(a, (LEFT, 1), (RIGHT, 0)) for a in range(2)]
    opp = [pair(a, (OPP, 0), (OPP, 1)) for a in range(2)]
    A, B, C, D = (0, 4), (4, 8), (8, 10), (10, 16)

    wait_partner(OWN, 0)
    wait_partner(OWN, 1)
    wait_q(1, 2, 3)
    block(own, [A])
    wait_q(P_Y2, P_Z2)
    for p in range(P_FAR, 16):
        send(q_copy(p))
    wait_ici(0)
    wait_ici(1)
    block(near0[0], [A])
    wait_q(4, 7)
    block(own, [B])
    block(near0[0], [B])
    wait_partner(LEFT, 0)
    wait_partner(RIGHT, 1)
    block(near0[1], [A, B])
    wait_ici(2)
    wait_ici(3)
    wait_q(8, 9)
    block(own + near0[0] + near0[1], [C])
    block(near1[0], [A, B, C])
    wait_partner(LEFT, 1)
    wait_partner(RIGHT, 0)
    block(near1[1], [A, B, C])
    wait_q(10, 11, 12, 13, 14, 15)
    for r in range(1, 16):
        zz, yy = plane_back(r)
        pl.semaphore_signal(ready, inc=1, device_id=dev(zz, yy, x, c), device_id_type=MESH)
    block(own, [D])
    wait_ici(4)
    wait_ici(5)
    block(near0[0] + near0[1] + near1[0] + near1[1], [D])
    block(opp[0], [A, B, C, D])
    wait_partner(OPP, 0)
    wait_partner(OPP, 1)
    block(opp[1], [A, B, C, D])

    def fold(side, core):
        a = jnp.maximum(best[side, core, 0], best[side, core, 1])
        return jnp.maximum(a, pltpu.roll(a, 4, 0))

    upper = iota((8, 2048), 0) < 4
    b = jnp.concatenate([jnp.where(upper, fold(side, 0), fold(side, 1)) for side in range(4)], axis=0)
    hi = b.astype(BF16)
    rest = b - hi.astype(F32)
    mid = rest.astype(BF16)
    low = (rest - mid.astype(F32)).astype(BF16)
    sums = jnp.dot(jnp.concatenate([hi, mid, low], axis=0), pick[...], preferred_element_type=F32)
    logits = ((sums[0:32] + sums[32:64]) + sums[64:96]) / temp_ref[0]
    lane = iota((32, 128), 1)
    sub = iota((32, 128), 0)
    lane1 = iota((1, 128), 1)
    my_slot = z * 4 + y
    my_line = x * 2 + c
    mine = (sub < 4) & (lane - my_slot * 4 == sub)
    pos_q = jnp.sum(jnp.where(mine, logits, 0.0), axis=0, keepdims=True)
    pos_total = jnp.sum(pos_q, axis=1, keepdims=True)
    m_row = jnp.max(logits, axis=0, keepdims=True)
    l_row = jnp.sum(jnp.exp(logits - m_row), axis=0, keepdims=True)
    qlane = lane < 64
    m_col = jnp.max(jnp.where(qlane, logits, -jnp.inf), axis=1, keepdims=True)
    l_col = jnp.sum(jnp.where(qlane, jnp.exp(logits - m_col), 0.0), axis=1, keepdims=True)
    side = sub // 8
    off = jnp.where(side == LEFT, 3, jnp.where(side == RIGHT, 1, jnp.where(side == OPP, 2, 0)))
    doc = ((x + off) & 3) * 8 + ((c + sub // 4) & 1) * 4 + (sub & 3)
    m_colr = jnp.sum(jnp.where(doc == lane - 64, m_col, 0.0), axis=0, keepdims=True)
    l_colr = jnp.sum(jnp.where(doc == lane - 64, l_col, 0.0), axis=0, keepdims=True)
    top_row = jnp.where(lane1 < 64, m_row, jnp.where(lane1 == 96, pos_total, m_colr))
    sum_row = jnp.where(lane1 < 64, l_row, l_colr)
    part[me] = jnp.concatenate([top_row, sum_row], axis=0)
    pl.semaphore_wait(ready, 15)

    def hops(r):
        return sum((0, 1, 2, 1)[(r >> b) & 3] for b in (1, 3, 5))

    for r in sorted(range(1, 128), key=hops, reverse=True):
        rdma(part.at[me], part.at[me], fs, fr, {'data': me ^ r}).start()
    for cp in sends:
        cp.wait_send()
    everyone = rdma(part.at[0:127], part.at[0:127], fs, fr, partner)
    everyone.wait_recv()
    tops = part[:, 0, :].reshape(16, 8, 128)
    adds = part[:, 1, :].reshape(16, 8, 128)
    mr = jnp.max(tops, axis=0)
    lse_row = mr + jnp.log(jnp.sum(adds * jnp.exp(tops - mr[None]), axis=0))
    mc = jnp.max(tops, axis=1, keepdims=True)
    lse_col = (mc + jnp.log(jnp.sum(adds * jnp.exp(tops - mc), axis=1, keepdims=True))).reshape(16, 128)
    lane8 = iota((8, 128), 1)
    lane16 = iota((16, 128), 1)
    row_sum = jnp.sum(jnp.where(lane8 < 64, lse_row, 0.0), axis=0, keepdims=True)
    col_sum = jnp.sum(jnp.where((lane16 >= 64) & (lane16 < 96), lse_col, 0.0), axis=0, keepdims=True)
    pos_sum = jnp.sum(jnp.sum(tops, axis=0), axis=0, keepdims=True)
    total = jnp.sum(row_sum + col_sum - jnp.where(lane1 == 96, 2.0 * pos_sum, 0.0), axis=1, keepdims=True)
    lm_ref[...] = jnp.broadcast_to(total / 1024.0, (1, 128))

    def to_front(v, start):
        return pltpu.roll(v, lax.rem(128 - start, 128), 1)

    pos_front = to_front(pos_q, my_slot * 4)
    my_row = jnp.sum(jnp.where(iota((8, 128), 0) == my_line, lse_row, 0.0), axis=0, keepdims=True)
    my_col = jnp.sum(jnp.where(iota((16, 128), 0) == my_slot, lse_col, 0.0), axis=0, keepdims=True)
    lq_ref[...] = (to_front(my_row, my_slot * 4) - pos_front)
    ld_ref[...] = (to_front(my_col, 64 + my_line * 4) - pos_front)
    everyone.wait_send()


def solution(mesh):
    batch_spec = P(('replica', 'data'))

    def local_loss(q_hidden, d_hidden, w_proj, q_mask, d_mask, temperature):
        vmem = pl.BlockSpec(memory_space=pltpu.VMEM)
        hbm = pl.BlockSpec(memory_space=pltpu.HBM)
        dma = pltpu.SemaphoreType.DMA
        lq, ld, lm = pl.pallas_call(
            kernel,
            out_shape=(jax.ShapeDtypeStruct((1, 128), F32),) * 3,
            in_specs=[hbm] * 5 + [pl.BlockSpec(memory_space=pltpu.SMEM)],
            out_specs=(vmem, vmem, vmem),
            scratch_shapes=[
                pltpu.VMEM((4, 32, 768), BF16),
                pltpu.VMEM((180, 4, 768), BF16),
                pltpu.VMEM((768, 128), BF16),
                pltpu.VMEM((4, 32), jnp.int32),
                pltpu.VMEM((4, 180), jnp.int32),
                dma((8,)),
                pltpu.VMEM((720, 128), F32),
                pltpu.VMEM((16, 128, 128), BF16),
                pltpu.VMEM((4, 2, 720, 128), BF16),
                pltpu.VMEM((4, 2, 2, 8, 2048), F32),
                pltpu.VMEM((2048, 128), BF16),
                pltpu.VMEM((128, 2, 128), F32),
                dma((16,)), dma((16,)), dma((6,)), dma((6,)), dma((8,)), dma((8,)), dma, dma,
                pltpu.SemaphoreType.REGULAR,
            ],
            compiler_params=pltpu.CompilerParams(collective_id=0, has_side_effects=True,
                                                 vmem_limit_bytes=48 * 1024 * 1024),
        )(*[pltpu.with_memory_space_constraint(a, pltpu.HBM)
            for a in (q_hidden, jnp.swapaxes(d_hidden, 0, 1), w_proj, q_mask, d_mask)], temperature.reshape(1))
        return lq[0, :4], ld[0, :4], lm[0, :1]

    return jax.shard_map(local_loss, mesh=mesh, in_specs=(batch_spec, batch_spec, P(), batch_spec, batch_spec, P()),
                         out_specs=(batch_spec, batch_spec, P('replica')), check_vma=False)
```

```python
import jax
import jax.numpy as jnp
from jax import lax
from jax.experimental import pallas as pl
from jax.experimental.pallas import tpu as pltpu
from jax.sharding import PartitionSpec as P

F32 = jnp.float32
BF16 = jnp.bfloat16
MESH = pl.DeviceIdType.MESH
HALF = 368
CUTS = (0, 46, 92, 136, 180)
Q_ORDER = (0, 1, 3, 4, 12, 2, 8, 5, 7, 13, 15, 6, 14, 9, 11, 10)
P_Y2, P_Z2, P_FAR = 5, 6, 11
OWN, LEFT, RIGHT, OPP = 0, 1, 2, 3


def unit_rows(raw):
    return raw / jnp.sqrt(jnp.sum(raw * raw, axis=-1, keepdims=True))


def iota(shape, axis):
    return lax.broadcasted_iota(jnp.int32, shape, axis)


def kernel(q_hbm, d_hbm, w_hbm, qm_hbm, dm_hbm, temp_ref, lq_ref, ld_ref, lm_ref,
           qh, dh, w, qm, dm, lsem, live, qbuf, dbuf, best, pick, part, qs, qr, ds_, dr, ps, pr, fs, fr, ready):
    me = lax.axis_index('data')
    c = lax.rem(me, 2)
    x = lax.rem(me // 2, 4)
    y = lax.rem(me // 8, 4)
    z = me // 32

    def dev(z_, y_, x_, c_):
        return {'data': ((z_ * 4 + y_) * 4 + x_) * 2 + c_}

    def plane(r):
        return lax.rem(z + r // 4, 4), lax.rem(y + r % 4, 4)

    def plane_back(r):
        return lax.rem(z + 4 - r // 4, 4), lax.rem(y + 4 - r % 4, 4)

    def line_back(r):
        return lax.rem(x + 4 - r // 2, 4), lax.rem(c + r % 2, 2)

    loads = [pltpu.make_async_copy(dm_hbm, dm, lsem.at[0]), pltpu.make_async_copy(w_hbm, w, lsem.at[1])]
    for i in range(4):
        rows = pl.ds(CUTS[i], CUTS[i + 1] - CUTS[i])
        loads.append(pltpu.make_async_copy(d_hbm.at[rows], dh.at[rows], lsem.at[2 + i]))
    loads += [pltpu.make_async_copy(q_hbm, qh, lsem.at[6]), pltpu.make_async_copy(qm_hbm, qm, lsem.at[7])]
    for cp in loads:
        cp.start()

    barrier = pltpu.get_barrier_semaphore()
    for r in Q_ORDER[1:P_FAR]:
        zz, yy = plane_back(r)
        pl.semaphore_signal(barrier, inc=1, device_id=dev(zz, yy, x, c), device_id_type=MESH)
    for r in range(1, 8):
        xx, cc = line_back(r)
        pl.semaphore_signal(barrier, inc=1, device_id=dev(z, y, xx, cc), device_id_type=MESH)

    loads[0].wait()
    d_col = jnp.transpose(jnp.concatenate([dm[...].astype(F32), jnp.zeros((4, 180), F32)], axis=0))
    for j in range(4):
        live[pl.ds(j, 180, stride=4), :] = jnp.broadcast_to(d_col[:, j:j + 1], (180, 128))
    valid = live[...].reshape(90, 8, 128) == 1.0
    token = (iota((720, 128), 0) // 4).reshape(90, 8, 128)
    first = jnp.min(jnp.where(valid, token, 1000), axis=0)
    first = jnp.minimum(first, pltpu.roll(first, 4, 0))
    for cp in loads[1:]:
        cp.wait()

    halves = [dh[0:92].reshape(HALF, 768), dh[92:180].reshape(720 - HALF, 768)]
    u = jnp.concatenate([unit_rows(jnp.dot(rows, w[...], preferred_element_type=F32)) for rows in halves], axis=0)
    u = u.reshape(90, 8, 128)
    vec = jnp.sum(jnp.where(token == first[None], u, 0.0), axis=0)
    vec = vec + pltpu.roll(vec, 4, 0)
    dbuf[OWN, 0] = jnp.where(valid, u, vec[None]).reshape(720, 128).astype(BF16)

    q_raw = jnp.dot(qh[...].reshape(128, 768), w[...], preferred_element_type=F32)
    q_col = jnp.transpose(jnp.concatenate([qm[...].astype(F32), jnp.zeros((4, 32), F32)], axis=0))
    q_valid = jnp.concatenate([q_col[:, i:i + 1] for i in range(4)], axis=0)
    qbuf[0] = jnp.where(q_valid == 1.0, unit_rows(q_raw), 0.0).astype(BF16)

    pl.semaphore_wait(barrier, 17)

    xr, xl = lax.rem(x + 1, 4), lax.rem(x + 3, 4)
    right, left, partner = dev(z, y, xr, c), dev(z, y, xl, c), dev(z, y, x, 1 - c)
    sends = []

    def rdma(src, dst, ssem, rsem, to):
        return pltpu.make_async_remote_copy(src, dst, ssem, rsem, device_id=to, device_id_type=MESH)

    def send(cp):
        cp.start()
        sends.append(cp)

    ICI = [(LEFT, 0), (RIGHT, 1), (LEFT, 1), (RIGHT, 0), (OPP, 0), (OPP, 1)]

    SPAN = (pl.ds(0, HALF), pl.ds(HALF, 720 - HALF))

    def to_right(src, h, i):
        return rdma(dbuf.at[src, 0, SPAN[h]], dbuf.at[ICI[i][0], 0, SPAN[h]], ds_.at[i], dr.at[i], right)

    def to_left(src, h, i):
        return rdma(dbuf.at[src, 0, SPAN[h]], dbuf.at[ICI[i][0], 0, SPAN[h]], ds_.at[i], dr.at[i], left)

    def to_partner(src, h):
        return rdma(dbuf.at[src, 0, SPAN[h]], dbuf.at[src, 1, SPAN[h]], ps.at[2 * src + h], pr.at[2 * src + h], partner)

    def q_copy(p):
        dz, dy = Q_ORDER[p] // 4, Q_ORDER[p] % 4
        src = 0
        if p >= P_FAR:
            if dy == 2:
                src, dy = P_Y2, 0
            else:
                src, dz = P_Z2, 0
        zz, yy = plane_back(4 * dz + dy)
        return rdma(qbuf.at[src], qbuf.at[p], qs.at[p], qr.at[p], dev(zz, yy, x, c))

    send(to_right(OWN, 0, 0))
    send(to_left(OWN, 1, 1))
    for p in (P_Y2, P_Z2, 1, 2, 3, 4):
        send(q_copy(p))
    send(to_partner(OWN, 0))
    send(to_partner(OWN, 1))
    send(to_right(OWN, 1, 2))
    send(to_left(OWN, 0, 3))
    for p in range(P_Z2 + 1, P_FAR):
        send(q_copy(p))

    def plane_slot(r):
        zz, yy = plane(r)
        return zz * 4 + yy

    tok = iota((128, 128), 0) // 32
    lanes = iota((128, 128), 1)
    for p in range(16):
        pick[p * 128:(p + 1) * 128, :] = (tok + 4 * plane_slot(Q_ORDER[p]) == lanes).astype(F32).astype(BF16)

    def wait_ici(i):
        side, h = ICI[i]
        to_right(OWN, h, i).wait_recv()
        if i == 0:
            send(to_right(LEFT, 0, 4))
        if i == 1:
            send(to_left(RIGHT, 1, 5))
        send(to_partner(side, h))

    def wait_partner(side, h):
        to_partner(side, h).wait_recv()

    def wait_q(*blocks):
        for p in blocks:
            q_copy(p).wait_recv()

    def block(pieces, chunks):
        lhs = jnp.concatenate([dbuf[side, core, SPAN[h], :] for side, core, h in pieces], axis=0)
        for lo, hi in chunks:
            width = (hi - lo) * 128
            rhs = qbuf[lo:hi].reshape(width, 128)
            sim = lax.dot_general(lhs, rhs, (((1,), (1,)), ((), ())), preferred_element_type=F32)
            at = 0
            for side, core, h in pieces:
                rows = HALF if h == 0 else 720 - HALF
                top = jnp.max(sim[at:at + rows].reshape(rows // 8, 8, width), axis=0)
                best[side, core, h, :, lo * 128:hi * 128] = top
                at += rows

    def pair(core, *halves):
        return [(side, core, h) for side, h in halves]

    own = pair(0, (OWN, 0), (OWN, 1)) + pair(1, (OWN, 0), (OWN, 1))
    near0 = [pair(a, (LEFT, 0), (RIGHT, 1)) for a in range(2)]
    near1 = [pair(a, (LEFT, 1), (RIGHT, 0)) for a in range(2)]
    opp = [pair(a, (OPP, 0), (OPP, 1)) for a in range(2)]
    A, B, C, D = (0, 4), (4, 8), (8, 10), (10, 16)

    wait_partner(OWN, 0)
    wait_partner(OWN, 1)
    wait_q(P_Y2, P_Z2)
    for p in range(P_FAR, 16):
        send(q_copy(p))
    wait_q(1, 2, 3)
    block(own, [A])
    wait_ici(0)
    wait_ici(1)
    block(near0[0], [A])
    wait_q(4, 7)
    block(own, [B])
    block(near0[0], [B])
    wait_partner(LEFT, 0)
    wait_partner(RIGHT, 1)
    block(near0[1], [A, B])
    wait_ici(2)
    wait_ici(3)
    wait_q(8, 9)
    block(own + near0[0] + near0[1], [C])
    block(near1[0], [A, B, C])
    wait_partner(LEFT, 1)
    wait_partner(RIGHT, 0)
    block(near1[1], [A, B, C])
    wait_q(10, 11, 12, 13, 14, 15)
    for r in range(1, 16):
        zz, yy = plane_back(r)
        pl.semaphore_signal(ready, inc=1, device_id=dev(zz, yy, x, c), device_id_type=MESH)
    wait_ici(4)
    wait_ici(5)
    block(own + near0[0] + near0[1] + near1[0] + near1[1], [D])
    block(opp[0], [A, B, C, D])
    wait_partner(OPP, 0)
    wait_partner(OPP, 1)
    block(opp[1], [A, B, C, D])

    def fold(side, core):
        a = jnp.maximum(best[side, core, 0], best[side, core, 1])
        return jnp.maximum(a, pltpu.roll(a, 4, 0))

    upper = iota((8, 2048), 0) < 4
    b = jnp.concatenate([jnp.where(upper, fold(side, 0), fold(side, 1)) for side in range(4)], axis=0)
    hi = b.astype(BF16)
    rest = b - hi.astype(F32)
    mid = rest.astype(BF16)
    low = (rest - mid.astype(F32)).astype(BF16)
    sums = jnp.dot(jnp.concatenate([hi, mid, low], axis=0), pick[...], preferred_element_type=F32)
    logits = ((sums[0:32] + sums[32:64]) + sums[64:96]) / temp_ref[0]
    lane = iota((32, 128), 1)
    sub = iota((32, 128), 0)
    lane1 = iota((1, 128), 1)
    my_slot = z * 4 + y
    my_line = x * 2 + c
    mine = (sub < 4) & (lane - my_slot * 4 == sub)
    pos_q = jnp.sum(jnp.where(mine, logits, 0.0), axis=0, keepdims=True)
    pos_total = jnp.sum(pos_q, axis=1, keepdims=True)
    m_row = jnp.max(logits, axis=0, keepdims=True)
    l_row = jnp.sum(jnp.exp(logits - m_row), axis=0, keepdims=True)
    qlane = lane < 64
    m_col = jnp.max(jnp.where(qlane, logits, -jnp.inf), axis=1, keepdims=True)
    l_col = jnp.sum(jnp.where(qlane, jnp.exp(logits - m_col), 0.0), axis=1, keepdims=True)
    side = sub // 8
    off = jnp.where(side == LEFT, 3, jnp.where(side == RIGHT, 1, jnp.where(side == OPP, 2, 0)))
    doc = ((x + off) & 3) * 8 + ((c + sub // 4) & 1) * 4 + (sub & 3)
    m_colr = jnp.sum(jnp.where(doc == lane - 64, m_col, 0.0), axis=0, keepdims=True)
    l_colr = jnp.sum(jnp.where(doc == lane - 64, l_col, 0.0), axis=0, keepdims=True)
    top_row = jnp.where(lane1 < 64, m_row, jnp.where(lane1 == 96, pos_total, m_colr))
    sum_row = jnp.where(lane1 < 64, l_row, l_colr)
    part[me] = jnp.concatenate([top_row, sum_row], axis=0)
    pl.semaphore_wait(ready, 15)

    def hops(r):
        return sum((0, 1, 2, 1)[(r >> b) & 3] for b in (1, 3, 5))

    for r in sorted(range(1, 128), key=hops, reverse=True):
        rdma(part.at[me], part.at[me], fs, fr, {'data': me ^ r}).start()
    for cp in sends:
        cp.wait_send()
    everyone = rdma(part.at[0:127], part.at[0:127], fs, fr, partner)
    everyone.wait_recv()
    tops = part[:, 0, :].reshape(16, 8, 128)
    adds = part[:, 1, :].reshape(16, 8, 128)
    mr = jnp.max(tops, axis=0)
    lse_row = mr + jnp.log(jnp.sum(adds * jnp.exp(tops - mr[None]), axis=0))
    mc = jnp.max(tops, axis=1, keepdims=True)
    lse_col = (mc + jnp.log(jnp.sum(adds * jnp.exp(tops - mc), axis=1, keepdims=True))).reshape(16, 128)
    lane8 = iota((8, 128), 1)
    lane16 = iota((16, 128), 1)
    row_sum = jnp.sum(jnp.where(lane8 < 64, lse_row, 0.0), axis=0, keepdims=True)
    col_sum = jnp.sum(jnp.where((lane16 >= 64) & (lane16 < 96), lse_col, 0.0), axis=0, keepdims=True)
    pos_sum = jnp.sum(jnp.sum(tops, axis=0), axis=0, keepdims=True)
    total = jnp.sum(row_sum + col_sum - jnp.where(lane1 == 96, 2.0 * pos_sum, 0.0), axis=1, keepdims=True)
    lm_ref[...] = jnp.broadcast_to(total / 1024.0, (1, 128))

    def to_front(v, start):
        return pltpu.roll(v, lax.rem(128 - start, 128), 1)

    pos_front = to_front(pos_q, my_slot * 4)
    my_row = jnp.sum(jnp.where(iota((8, 128), 0) == my_line, lse_row, 0.0), axis=0, keepdims=True)
    my_col = jnp.sum(jnp.where(iota((16, 128), 0) == my_slot, lse_col, 0.0), axis=0, keepdims=True)
    lq_ref[...] = (to_front(my_row, my_slot * 4) - pos_front)
    ld_ref[...] = (to_front(my_col, 64 + my_line * 4) - pos_front)
    everyone.wait_send()


def solution(mesh):
    batch_spec = P(('replica', 'data'))

    def local_loss(q_hidden, d_hidden, w_proj, q_mask, d_mask, temperature):
        vmem = pl.BlockSpec(memory_space=pltpu.VMEM)
        hbm = pl.BlockSpec(memory_space=pltpu.HBM)
        dma = pltpu.SemaphoreType.DMA
        lq, ld, lm = pl.pallas_call(
            kernel,
            out_shape=(jax.ShapeDtypeStruct((1, 128), F32),) * 3,
            in_specs=[hbm] * 5 + [pl.BlockSpec(memory_space=pltpu.SMEM)],
            out_specs=(vmem, vmem, vmem),
            scratch_shapes=[
                pltpu.VMEM((4, 32, 768), BF16),
                pltpu.VMEM((180, 4, 768), BF16),
                pltpu.VMEM((768, 128), BF16),
                pltpu.VMEM((4, 32), jnp.int32),
                pltpu.VMEM((4, 180), jnp.int32),
                dma((8,)),
                pltpu.VMEM((720, 128), F32),
                pltpu.VMEM((16, 128, 128), BF16),
                pltpu.VMEM((4, 2, 720, 128), BF16),
                pltpu.VMEM((4, 2, 2, 8, 2048), F32),
                pltpu.VMEM((2048, 128), BF16),
                pltpu.VMEM((128, 2, 128), F32),
                dma((16,)), dma((16,)), dma((6,)), dma((6,)), dma((8,)), dma((8,)), dma, dma,
                pltpu.SemaphoreType.REGULAR,
            ],
            compiler_params=pltpu.CompilerParams(collective_id=0, has_side_effects=True,
                                                 vmem_limit_bytes=48 * 1024 * 1024),
        )(*[pltpu.with_memory_space_constraint(a, pltpu.HBM)
            for a in (q_hidden, jnp.swapaxes(d_hidden, 0, 1), w_proj, q_mask, d_mask)], temperature.reshape(1))
        return lq[0, :4], ld[0, :4], lm[0, :1]

    return jax.shard_map(local_loss, mesh=mesh, in_specs=(batch_spec, batch_spec, P(), batch_spec, batch_spec, P()),
                         out_specs=(batch_spec, batch_spec, P('replica')), check_vma=False)
```

```python
import jax
import jax.numpy as jnp
from jax import lax
from jax.experimental import pallas as pl
from jax.experimental.pallas import tpu as pltpu
from jax.sharding import PartitionSpec as P

F32 = jnp.float32
BF16 = jnp.bfloat16
MESH = pl.DeviceIdType.MESH
HALF = 368
CUTS = (0, 46, 92, 136, 180)
Q_ORDER = (0, 1, 3, 4, 12, 2, 8, 5, 7, 13, 15, 6, 14, 9, 11, 10)
P_Y2, P_Z2, P_FAR = 5, 6, 11
OWN, LEFT, RIGHT, OPP = 0, 1, 2, 3


def unit_rows(raw):
    return raw / jnp.sqrt(jnp.sum(raw * raw, axis=-1, keepdims=True))


def iota(shape, axis):
    return lax.broadcasted_iota(jnp.int32, shape, axis)


def kernel(q_hbm, d_hbm, w_hbm, qm_hbm, dm_hbm, temp_ref, lq_ref, ld_ref, lm_ref,
           qh, dh, w, qm, dm, lsem, live, qbuf, dbuf, best, pick, part, qs, qr, ds_, dr, ps, pr, fs, fr, ready):
    me = lax.axis_index('data')
    c = lax.rem(me, 2)
    x = lax.rem(me // 2, 4)
    y = lax.rem(me // 8, 4)
    z = me // 32

    def dev(z_, y_, x_, c_):
        return {'data': ((z_ * 4 + y_) * 4 + x_) * 2 + c_}

    def plane(r):
        return lax.rem(z + r // 4, 4), lax.rem(y + r % 4, 4)

    def plane_back(r):
        return lax.rem(z + 4 - r // 4, 4), lax.rem(y + 4 - r % 4, 4)

    def line_back(r):
        return lax.rem(x + 4 - r // 2, 4), lax.rem(c + r % 2, 2)

    loads = [pltpu.make_async_copy(dm_hbm, dm, lsem.at[0]), pltpu.make_async_copy(w_hbm, w, lsem.at[1])]
    for i in range(4):
        rows = pl.ds(CUTS[i], CUTS[i + 1] - CUTS[i])
        loads.append(pltpu.make_async_copy(d_hbm.at[rows], dh.at[rows], lsem.at[2 + i]))
    loads += [pltpu.make_async_copy(q_hbm, qh, lsem.at[6]), pltpu.make_async_copy(qm_hbm, qm, lsem.at[7])]
    for cp in loads:
        cp.start()

    barrier = pltpu.get_barrier_semaphore()
    for r in Q_ORDER[1:P_FAR]:
        zz, yy = plane_back(r)
        pl.semaphore_signal(barrier, inc=1, device_id=dev(zz, yy, x, c), device_id_type=MESH)
    for r in range(1, 8):
        xx, cc = line_back(r)
        pl.semaphore_signal(barrier, inc=1, device_id=dev(z, y, xx, cc), device_id_type=MESH)

    loads[0].wait()
    d_col = jnp.transpose(jnp.concatenate([dm[...].astype(F32), jnp.zeros((4, 180), F32)], axis=0))
    for j in range(4):
        live[pl.ds(j, 180, stride=4), :] = jnp.broadcast_to(d_col[:, j:j + 1], (180, 128))
    valid = live[...].reshape(90, 8, 128) == 1.0
    token = (iota((720, 128), 0) // 4).reshape(90, 8, 128)
    first = jnp.min(jnp.where(valid, token, 1000), axis=0)
    first = jnp.minimum(first, pltpu.roll(first, 4, 0))
    for cp in loads[1:]:
        cp.wait()

    halves = [dh[0:92].reshape(HALF, 768), dh[92:180].reshape(720 - HALF, 768)]
    u = jnp.concatenate([unit_rows(jnp.dot(rows, w[...], preferred_element_type=F32)) for rows in halves], axis=0)
    u = u.reshape(90, 8, 128)
    vec = jnp.sum(jnp.where(token == first[None], u, 0.0), axis=0)
    vec = vec + pltpu.roll(vec, 4, 0)
    dbuf[OWN, 0] = jnp.where(valid, u, vec[None]).reshape(720, 128).astype(BF16)

    q_raw = jnp.dot(qh[...].reshape(128, 768), w[...], preferred_element_type=F32)
    q_col = jnp.transpose(jnp.concatenate([qm[...].astype(F32), jnp.zeros((4, 32), F32)], axis=0))
    q_valid = jnp.concatenate([q_col[:, i:i + 1] for i in range(4)], axis=0)
    qbuf[0] = jnp.where(q_valid == 1.0, unit_rows(q_raw), 0.0).astype(BF16)

    pl.semaphore_wait(barrier, 17)

    xr, xl = lax.rem(x + 1, 4), lax.rem(x + 3, 4)
    right, left, partner = dev(z, y, xr, c), dev(z, y, xl, c), dev(z, y, x, 1 - c)
    sends = []

    def rdma(src, dst, ssem, rsem, to):
        return pltpu.make_async_remote_copy(src, dst, ssem, rsem, device_id=to, device_id_type=MESH)

    def send(cp):
        cp.start()
        sends.append(cp)

    ICI = [(LEFT, 1), (RIGHT, 0)]

    SPAN = (pl.ds(0, HALF), pl.ds(HALF, 720 - HALF))

    def to_right(src, h, i):
        return rdma(dbuf.at[src, 0, SPAN[h]], dbuf.at[ICI[i][0], 0, SPAN[h]], ds_.at[i], dr.at[i], right)

    def to_left(src, h, i):
        return rdma(dbuf.at[src, 0, SPAN[h]], dbuf.at[ICI[i][0], 0, SPAN[h]], ds_.at[i], dr.at[i], left)

    PARTS = ((pl.ds(0, 192), pl.ds(192, 176)), (pl.ds(HALF, 176), pl.ds(HALF + 176, 176)))

    def along(src, h, part):
        dst = OPP if src != OWN else (LEFT, RIGHT)[h]
        k = h + 2 * part + (6 if src != OWN else 2)
        rows = PARTS[h][part]
        return rdma(dbuf.at[src, 0, rows], dbuf.at[dst, 0, rows], ds_.at[k], dr.at[k], (right, left)[h])

    def to_partner(src, h):
        return rdma(dbuf.at[src, 0, SPAN[h]], dbuf.at[src, 1, SPAN[h]], ps.at[2 * src + h], pr.at[2 * src + h], partner)

    def q_copy(p):
        dz, dy = Q_ORDER[p] // 4, Q_ORDER[p] % 4
        src = 0
        if p >= P_FAR:
            if dy == 2:
                src, dy = P_Y2, 0
            else:
                src, dz = P_Z2, 0
        zz, yy = plane_back(4 * dz + dy)
        return rdma(qbuf.at[src], qbuf.at[p], qs.at[p], qr.at[p], dev(zz, yy, x, c))

    for part_ in range(2):
        send(along(OWN, 0, part_))
        send(along(OWN, 1, part_))
    for p in (P_Y2, P_Z2, 1, 2, 3, 4):
        send(q_copy(p))
    send(to_partner(OWN, 0))
    send(to_partner(OWN, 1))
    send(to_right(OWN, 1, 0))
    send(to_left(OWN, 0, 1))
    for p in range(P_Z2 + 1, P_FAR):
        send(q_copy(p))

    def plane_slot(r):
        zz, yy = plane(r)
        return zz * 4 + yy

    tok = iota((128, 128), 0) // 32
    lanes = iota((128, 128), 1)
    for p in range(16):
        pick[p * 128:(p + 1) * 128, :] = (tok + 4 * plane_slot(Q_ORDER[p]) == lanes).astype(F32).astype(BF16)

    def wait_first(part_):
        for h in range(2):
            along(OWN, h, part_).wait_recv()
            send(along((LEFT, RIGHT)[h], h, part_))
            if part_ == 1:
                send(to_partner((LEFT, RIGHT)[h], h))

    def wait_second():
        for i, (side, h) in enumerate(ICI):
            to_right(OWN, h, i).wait_recv()
            send(to_partner(side, h))

    def wait_opp():
        for h in range(2):
            for part_ in range(2):
                along((LEFT, RIGHT)[h], h, part_).wait_recv()
            send(to_partner(OPP, h))

    def wait_partner(side, h):
        to_partner(side, h).wait_recv()

    def wait_q(*blocks):
        for p in blocks:
            q_copy(p).wait_recv()

    def block(pieces, chunks):
        lhs = jnp.concatenate([dbuf[side, core, SPAN[h], :] for side, core, h in pieces], axis=0)
        for lo, hi in chunks:
            width = (hi - lo) * 128
            rhs = qbuf[lo:hi].reshape(width, 128)
            sim = lax.dot_general(lhs, rhs, (((1,), (1,)), ((), ())), preferred_element_type=F32)
            at = 0
            for side, core, h in pieces:
                rows = HALF if h == 0 else 720 - HALF
                top = jnp.max(sim[at:at + rows].reshape(rows // 8, 8, width), axis=0)
                best[side, core, h, :, lo * 128:hi * 128] = top
                at += rows

    def pair(core, *halves):
        return [(side, core, h) for side, h in halves]

    own = pair(0, (OWN, 0), (OWN, 1)) + pair(1, (OWN, 0), (OWN, 1))
    near0 = [pair(a, (LEFT, 0), (RIGHT, 1)) for a in range(2)]
    near1 = [pair(a, (LEFT, 1), (RIGHT, 0)) for a in range(2)]
    opp = [pair(a, (OPP, 0), (OPP, 1)) for a in range(2)]
    A, B, C, D = (0, 4), (4, 8), (8, 10), (10, 16)

    wait_partner(OWN, 0)
    wait_partner(OWN, 1)
    wait_first(0)
    wait_q(P_Y2, P_Z2)
    for p in range(P_FAR, 16):
        send(q_copy(p))
    wait_q(1, 2, 3)
    block(own, [A])
    wait_first(1)
    block(near0[0], [A])
    wait_q(4, 7)
    block(own, [B])
    block(near0[0], [B])
    wait_partner(LEFT, 0)
    wait_partner(RIGHT, 1)
    block(near0[1], [A, B])
    wait_second()
    wait_q(8, 9)
    block(own + near0[0] + near0[1], [C])
    block(near1[0], [A, B, C])
    wait_partner(LEFT, 1)
    wait_partner(RIGHT, 0)
    block(near1[1], [A, B, C])
    wait_q(10, 11, 12, 13, 14, 15)
    for r in range(1, 16):
        zz, yy = plane_back(r)
        pl.semaphore_signal(ready, inc=1, device_id=dev(zz, yy, x, c), device_id_type=MESH)
    wait_opp()
    block(own + near0[0] + near0[1] + near1[0] + near1[1], [D])
    block(opp[0], [A, B, C, D])
    wait_partner(OPP, 0)
    wait_partner(OPP, 1)
    block(opp[1], [A, B, C, D])

    def fold(side, core):
        a = jnp.maximum(best[side, core, 0], best[side, core, 1])
        return jnp.maximum(a, pltpu.roll(a, 4, 0))

    upper = iota((8, 2048), 0) < 4
    b = jnp.concatenate([jnp.where(upper, fold(side, 0), fold(side, 1)) for side in range(4)], axis=0)
    hi = b.astype(BF16)
    rest = b - hi.astype(F32)
    mid = rest.astype(BF16)
    low = (rest - mid.astype(F32)).astype(BF16)
    sums = jnp.dot(jnp.concatenate([hi, mid, low], axis=0), pick[...], preferred_element_type=F32)
    logits = ((sums[0:32] + sums[32:64]) + sums[64:96]) / temp_ref[0]
    lane = iota((32, 128), 1)
    sub = iota((32, 128), 0)
    lane1 = iota((1, 128), 1)
    my_slot = z * 4 + y
    my_line = x * 2 + c
    mine = (sub < 4) & (lane - my_slot * 4 == sub)
    pos_q = jnp.sum(jnp.where(mine, logits, 0.0), axis=0, keepdims=True)
    pos_total = jnp.sum(pos_q, axis=1, keepdims=True)
    m_row = jnp.max(logits, axis=0, keepdims=True)
    l_row = jnp.sum(jnp.exp(logits - m_row), axis=0, keepdims=True)
    qlane = lane < 64
    m_col = jnp.max(jnp.where(qlane, logits, -jnp.inf), axis=1, keepdims=True)
    l_col = jnp.sum(jnp.where(qlane, jnp.exp(logits - m_col), 0.0), axis=1, keepdims=True)
    side = sub // 8
    off = jnp.where(side == LEFT, 3, jnp.where(side == RIGHT, 1, jnp.where(side == OPP, 2, 0)))
    doc = ((x + off) & 3) * 8 + ((c + sub // 4) & 1) * 4 + (sub & 3)
    m_colr = jnp.sum(jnp.where(doc == lane - 64, m_col, 0.0), axis=0, keepdims=True)
    l_colr = jnp.sum(jnp.where(doc == lane - 64, l_col, 0.0), axis=0, keepdims=True)
    top_row = jnp.where(lane1 < 64, m_row, jnp.where(lane1 == 96, pos_total, m_colr))
    sum_row = jnp.where(lane1 < 64, l_row, l_colr)
    part[me] = jnp.concatenate([top_row, sum_row], axis=0)
    pl.semaphore_wait(ready, 15)

    def hops(r):
        return sum((0, 1, 2, 1)[(r >> b) & 3] for b in (1, 3, 5))

    for r in sorted(range(1, 128), key=hops, reverse=True):
        rdma(part.at[me], part.at[me], fs, fr, {'data': me ^ r}).start()
    for cp in sends:
        cp.wait_send()
    everyone = rdma(part.at[0:127], part.at[0:127], fs, fr, partner)
    everyone.wait_recv()
    tops = part[:, 0, :].reshape(16, 8, 128)
    adds = part[:, 1, :].reshape(16, 8, 128)
    mr = jnp.max(tops, axis=0)
    lse_row = mr + jnp.log(jnp.sum(adds * jnp.exp(tops - mr[None]), axis=0))
    mc = jnp.max(tops, axis=1, keepdims=True)
    lse_col = (mc + jnp.log(jnp.sum(adds * jnp.exp(tops - mc), axis=1, keepdims=True))).reshape(16, 128)
    lane8 = iota((8, 128), 1)
    lane16 = iota((16, 128), 1)
    row_sum = jnp.sum(jnp.where(lane8 < 64, lse_row, 0.0), axis=0, keepdims=True)
    col_sum = jnp.sum(jnp.where((lane16 >= 64) & (lane16 < 96), lse_col, 0.0), axis=0, keepdims=True)
    pos_sum = jnp.sum(jnp.sum(tops, axis=0), axis=0, keepdims=True)
    total = jnp.sum(row_sum + col_sum - jnp.where(lane1 == 96, 2.0 * pos_sum, 0.0), axis=1, keepdims=True)
    lm_ref[...] = jnp.broadcast_to(total / 1024.0, (1, 128))

    def to_front(v, start):
        return pltpu.roll(v, lax.rem(128 - start, 128), 1)

    pos_front = to_front(pos_q, my_slot * 4)
    my_row = jnp.sum(jnp.where(iota((8, 128), 0) == my_line, lse_row, 0.0), axis=0, keepdims=True)
    my_col = jnp.sum(jnp.where(iota((16, 128), 0) == my_slot, lse_col, 0.0), axis=0, keepdims=True)
    lq_ref[...] = (to_front(my_row, my_slot * 4) - pos_front)
    ld_ref[...] = (to_front(my_col, 64 + my_line * 4) - pos_front)
    everyone.wait_send()


def solution(mesh):
    batch_spec = P(('replica', 'data'))

    def local_loss(q_hidden, d_hidden, w_proj, q_mask, d_mask, temperature):
        vmem = pl.BlockSpec(memory_space=pltpu.VMEM)
        hbm = pl.BlockSpec(memory_space=pltpu.HBM)
        dma = pltpu.SemaphoreType.DMA
        lq, ld, lm = pl.pallas_call(
            kernel,
            out_shape=(jax.ShapeDtypeStruct((1, 128), F32),) * 3,
            in_specs=[hbm] * 5 + [pl.BlockSpec(memory_space=pltpu.SMEM)],
            out_specs=(vmem, vmem, vmem),
            scratch_shapes=[
                pltpu.VMEM((4, 32, 768), BF16),
                pltpu.VMEM((180, 4, 768), BF16),
                pltpu.VMEM((768, 128), BF16),
                pltpu.VMEM((4, 32), jnp.int32),
                pltpu.VMEM((4, 180), jnp.int32),
                dma((8,)),
                pltpu.VMEM((720, 128), F32),
                pltpu.VMEM((16, 128, 128), BF16),
                pltpu.VMEM((4, 2, 720, 128), BF16),
                pltpu.VMEM((4, 2, 2, 8, 2048), F32),
                pltpu.VMEM((2048, 128), BF16),
                pltpu.VMEM((128, 2, 128), F32),
                dma((16,)), dma((16,)), dma((10,)), dma((10,)), dma((8,)), dma((8,)), dma, dma,
                pltpu.SemaphoreType.REGULAR,
            ],
            compiler_params=pltpu.CompilerParams(collective_id=0, has_side_effects=True,
                                                 vmem_limit_bytes=48 * 1024 * 1024),
        )(*[pltpu.with_memory_space_constraint(a, pltpu.HBM)
            for a in (q_hidden, jnp.swapaxes(d_hidden, 0, 1), w_proj, q_mask, d_mask)], temperature.reshape(1))
        return lq[0, :4], ld[0, :4], lm[0, :1]

    return jax.shard_map(local_loss, mesh=mesh, in_specs=(batch_spec, batch_spec, P(), batch_spec, batch_spec, P()),
                         out_specs=(batch_spec, batch_spec, P('replica')), check_vma=False)
```

```python
import jax
import jax.numpy as jnp
from jax import lax
from jax.experimental import pallas as pl
from jax.experimental.pallas import tpu as pltpu
from jax.sharding import PartitionSpec as P

F32 = jnp.float32
BF16 = jnp.bfloat16
MESH = pl.DeviceIdType.MESH
HALF = 368
CUTS = (0, 46, 92, 136, 180)
Q_ORDER = (0, 1, 3, 4, 12, 2, 8, 5, 7, 13, 15, 6, 14, 9, 11, 10)
P_Y2, P_Z2, P_FAR = 5, 6, 11
OWN, LEFT, RIGHT, OPP = 0, 1, 2, 3


def unit_rows(raw):
    return raw / jnp.sqrt(jnp.sum(raw * raw, axis=-1, keepdims=True))


def iota(shape, axis):
    return lax.broadcasted_iota(jnp.int32, shape, axis)


def kernel(q_hbm, d_hbm, w_hbm, qm_hbm, dm_hbm, temp_ref, lq_ref, ld_ref, lm_ref,
           qh, dh, w, qm, dm, lsem, live, qbuf, dbuf, best, pick, part, qs, qr, ds_, dr, ps, pr, fs, fr, ready):
    me = lax.axis_index('data')
    c = lax.rem(me, 2)
    x = lax.rem(me // 2, 4)
    y = lax.rem(me // 8, 4)
    z = me // 32

    def dev(z_, y_, x_, c_):
        return {'data': ((z_ * 4 + y_) * 4 + x_) * 2 + c_}

    def plane(r):
        return lax.rem(z + r // 4, 4), lax.rem(y + r % 4, 4)

    def plane_back(r):
        return lax.rem(z + 4 - r // 4, 4), lax.rem(y + 4 - r % 4, 4)

    def line_back(r):
        return lax.rem(x + 4 - r // 2, 4), lax.rem(c + r % 2, 2)

    loads = [pltpu.make_async_copy(dm_hbm, dm, lsem.at[0]), pltpu.make_async_copy(w_hbm, w, lsem.at[1])]
    for i in range(4):
        rows = pl.ds(CUTS[i], CUTS[i + 1] - CUTS[i])
        loads.append(pltpu.make_async_copy(d_hbm.at[rows], dh.at[rows], lsem.at[2 + i]))
    loads += [pltpu.make_async_copy(q_hbm, qh, lsem.at[6]), pltpu.make_async_copy(qm_hbm, qm, lsem.at[7])]
    for cp in loads:
        cp.start()

    barrier = pltpu.get_barrier_semaphore()
    for r in Q_ORDER[1:P_FAR]:
        zz, yy = plane_back(r)
        pl.semaphore_signal(barrier, inc=1, device_id=dev(zz, yy, x, c), device_id_type=MESH)
    for r in range(1, 8):
        xx, cc = line_back(r)
        pl.semaphore_signal(barrier, inc=1, device_id=dev(z, y, xx, cc), device_id_type=MESH)

    loads[0].wait()
    d_col = jnp.transpose(jnp.concatenate([dm[...].astype(F32), jnp.zeros((4, 180), F32)], axis=0))
    for j in range(4):
        live[pl.ds(j, 180, stride=4), :] = jnp.broadcast_to(d_col[:, j:j + 1], (180, 128))
    valid = live[0:720].reshape(90, 8, 128) == 1.0
    token = (iota((720, 128), 0) // 4).reshape(90, 8, 128)
    first = jnp.min(jnp.where(valid, token, 1000), axis=0)
    first = jnp.minimum(first, pltpu.roll(first, 4, 0))
    for cp in loads[1:]:
        cp.wait()

    halves = [dh[0:92].reshape(HALF, 768), dh[92:180].reshape(720 - HALF, 768)]
    u = jnp.concatenate([unit_rows(jnp.dot(rows, w[...], preferred_element_type=F32)) for rows in halves], axis=0)
    u = u.reshape(90, 8, 128)
    vec = jnp.sum(jnp.where(token == first[None], u, 0.0), axis=0)
    vec = vec + pltpu.roll(vec, 4, 0)
    dbuf[OWN, 0] = jnp.where(valid, u, vec[None]).reshape(720, 128).astype(BF16)

    q_raw = jnp.dot(qh[...].reshape(128, 768), w[...], preferred_element_type=F32)
    q_col = jnp.transpose(jnp.concatenate([qm[...].astype(F32), jnp.zeros((4, 32), F32)], axis=0))
    q_valid = jnp.concatenate([q_col[:, i:i + 1] for i in range(4)], axis=0)
    qbuf[0] = jnp.where(q_valid == 1.0, unit_rows(q_raw), 0.0).astype(BF16)

    pl.semaphore_wait(barrier, 17)

    xr, xl = lax.rem(x + 1, 4), lax.rem(x + 3, 4)
    right, left, partner = dev(z, y, xr, c), dev(z, y, xl, c), dev(z, y, x, 1 - c)
    sends = []

    def rdma(src, dst, ssem, rsem, to):
        return pltpu.make_async_remote_copy(src, dst, ssem, rsem, device_id=to, device_id_type=MESH)

    def send(cp):
        cp.start()
        sends.append(cp)

    ICI = [(LEFT, 1), (RIGHT, 0)]

    SPAN = (pl.ds(0, HALF), pl.ds(HALF, 720 - HALF))

    def to_right(src, h, i):
        return rdma(dbuf.at[src, 0, SPAN[h]], dbuf.at[ICI[i][0], 0, SPAN[h]], ds_.at[i], dr.at[i], right)

    def to_left(src, h, i):
        return rdma(dbuf.at[src, 0, SPAN[h]], dbuf.at[ICI[i][0], 0, SPAN[h]], ds_.at[i], dr.at[i], left)

    PARTS = ((pl.ds(0, 192), pl.ds(192, 176)), (pl.ds(HALF, 176), pl.ds(HALF + 176, 176)))

    def along(src, h, part):
        dst = OPP if src != OWN else (LEFT, RIGHT)[h]
        k = h + 2 * part + (6 if src != OWN else 2)
        rows = PARTS[h][part]
        return rdma(dbuf.at[src, 0, rows], dbuf.at[dst, 0, rows], ds_.at[k], dr.at[k], (right, left)[h])

    def to_partner(src, h):
        return rdma(dbuf.at[src, 0, SPAN[h]], dbuf.at[src, 1, SPAN[h]], ps.at[2 * src + h], pr.at[2 * src + h], partner)

    def q_copy(p):
        dz, dy = Q_ORDER[p] // 4, Q_ORDER[p] % 4
        src = 0
        if p >= P_FAR:
            if dy == 2:
                src, dy = P_Y2, 0
            else:
                src, dz = P_Z2, 0
        zz, yy = plane_back(4 * dz + dy)
        return rdma(qbuf.at[src], qbuf.at[p], qs.at[p], qr.at[p], dev(zz, yy, x, c))

    for part_ in range(2):
        send(along(OWN, 0, part_))
        send(along(OWN, 1, part_))
    for p in (P_Y2, P_Z2, 1, 2, 3, 4):
        send(q_copy(p))
    send(to_partner(OWN, 0))
    send(to_partner(OWN, 1))
    send(to_right(OWN, 1, 0))
    send(to_left(OWN, 0, 1))
    for p in range(P_Z2 + 1, P_FAR):
        send(q_copy(p))

    def plane_slot(r):
        zz, yy = plane(r)
        return zz * 4 + yy

    tok = iota((128, 128), 0) // 32
    lanes = iota((128, 128), 1)
    for p in range(16):
        pick[p * 128:(p + 1) * 128, :] = (tok + 4 * plane_slot(Q_ORDER[p]) == lanes).astype(F32).astype(BF16)

    def wait_first(part_):
        for h in range(2):
            along(OWN, h, part_).wait_recv()
            send(along((LEFT, RIGHT)[h], h, part_))
            if part_ == 1:
                send(to_partner((LEFT, RIGHT)[h], h))

    def wait_second():
        for i, (side, h) in enumerate(ICI):
            to_right(OWN, h, i).wait_recv()
            send(to_partner(side, h))

    def wait_opp():
        for h in range(2):
            for part_ in range(2):
                along((LEFT, RIGHT)[h], h, part_).wait_recv()
            send(to_partner(OPP, h))

    def wait_partner(side, h):
        to_partner(side, h).wait_recv()

    def wait_q(*blocks):
        for p in blocks:
            q_copy(p).wait_recv()

    def block(pieces, chunks):
        lhs = jnp.concatenate([dbuf[side, core, SPAN[h], :] for side, core, h in pieces], axis=0)
        for lo, hi in chunks:
            width = (hi - lo) * 128
            rhs = qbuf[lo:hi].reshape(width, 128)
            sim = lax.dot_general(lhs, rhs, (((1,), (1,)), ((), ())), preferred_element_type=F32)
            at = 0
            for side, core, h in pieces:
                rows = HALF if h == 0 else 720 - HALF
                top = jnp.max(sim[at:at + rows].reshape(rows // 8, 8, width), axis=0)
                best[side, core, h, :, lo * 128:hi * 128] = top
                at += rows

    def pair(core, *halves):
        return [(side, core, h) for side, h in halves]

    own = pair(0, (OWN, 0), (OWN, 1)) + pair(1, (OWN, 0), (OWN, 1))
    near0 = [pair(a, (LEFT, 0), (RIGHT, 1)) for a in range(2)]
    near1 = [pair(a, (LEFT, 1), (RIGHT, 0)) for a in range(2)]
    opp = [pair(a, (OPP, 0), (OPP, 1)) for a in range(2)]
    A, B, C, D = (0, 4), (4, 8), (8, 10), (10, 16)

    wait_partner(OWN, 0)
    wait_partner(OWN, 1)
    wait_first(0)
    wait_q(P_Y2, P_Z2)
    for p in range(P_FAR, 16):
        send(q_copy(p))
    wait_q(1, 2, 3)
    block(own, [A])
    wait_first(1)
    block(near0[0], [A])
    wait_q(4, 7)
    block(own, [B])
    block(near0[0], [B])
    wait_partner(LEFT, 0)
    wait_partner(RIGHT, 1)
    block(near0[1], [A, B])
    wait_second()
    wait_q(8, 9)
    block(own + near0[0] + near0[1], [C])
    block(near1[0], [A, B, C])
    wait_partner(LEFT, 1)
    wait_partner(RIGHT, 0)
    block(near1[1], [A, B, C])
    wait_q(10, 11, 12, 13, 14, 15)
    for r in range(1, 16):
        zz, yy = plane_back(r)
        pl.semaphore_signal(ready, inc=1, device_id=dev(zz, yy, x, c), device_id_type=MESH)
    wait_opp()
    block(own + near0[0] + near0[1] + near1[0] + near1[1], [D])
    block(opp[0], [A, B, C, D])
    wait_partner(OPP, 0)
    wait_partner(OPP, 1)
    block(opp[1], [A, B, C, D])

    def fold(side, core):
        a = jnp.maximum(best[side, core, 0], best[side, core, 1])
        return jnp.maximum(a, pltpu.roll(a, 4, 0))

    upper = iota((8, 2048), 0) < 4
    b = jnp.concatenate([jnp.where(upper, fold(side, 0), fold(side, 1)) for side in range(4)], axis=0)
    hi = b.astype(BF16)
    rest = b - hi.astype(F32)
    mid = rest.astype(BF16)
    low = (rest - mid.astype(F32)).astype(BF16)
    sums = jnp.dot(jnp.concatenate([hi, mid, low], axis=0), pick[...], preferred_element_type=F32)
    logits = ((sums[0:32] + sums[32:64]) + sums[64:96]) / temp_ref[0]
    lane = iota((32, 128), 1)
    sub = iota((32, 128), 0)
    lane1 = iota((1, 128), 1)
    my_slot = z * 4 + y
    my_line = x * 2 + c
    mine = (sub < 4) & (lane - my_slot * 4 == sub)
    pos_q = jnp.sum(jnp.where(mine, logits, 0.0), axis=0, keepdims=True)
    pos_total = jnp.sum(pos_q, axis=1, keepdims=True)
    m_row = jnp.max(logits, axis=0, keepdims=True)
    l_row = jnp.sum(jnp.exp(logits - m_row), axis=0, keepdims=True)
    qlane = lane < 64
    m_col = jnp.max(jnp.where(qlane, logits, -jnp.inf), axis=1, keepdims=True)
    l_col = jnp.sum(jnp.where(qlane, jnp.exp(logits - m_col), 0.0), axis=1, keepdims=True)
    side = sub // 8
    off = jnp.where(side == LEFT, 3, jnp.where(side == RIGHT, 1, jnp.where(side == OPP, 2, 0)))
    doc = ((x + off) & 3) * 8 + ((c + sub // 4) & 1) * 4 + (sub & 3)
    m_colr = jnp.sum(jnp.where(doc == lane - 64, m_col, 0.0), axis=0, keepdims=True)
    l_colr = jnp.sum(jnp.where(doc == lane - 64, l_col, 0.0), axis=0, keepdims=True)
    top_row = jnp.where(lane1 < 64, m_row, jnp.where(lane1 == 96, pos_total, m_colr))
    sum_row = jnp.where(lane1 < 64, l_row, l_colr)
    part[me] = jnp.concatenate([top_row, sum_row], axis=0)
    pl.semaphore_wait(ready, 15)

    def hops(r):
        return sum((0, 1, 2, 1)[(r >> b) & 3] for b in (1, 3, 5))

    for r in sorted(range(1, 128), key=hops, reverse=True):
        rdma(part.at[me], part.at[me], fs, fr, {'data': me ^ r}).start()
    for cp in sends:
        cp.wait_send()
    everyone = rdma(part.at[0:127], part.at[0:127], fs, fr, partner)
    everyone.wait_recv()
    tops = part[:, 0, :].reshape(16, 8, 128)
    adds = part[:, 1, :].reshape(16, 8, 128)
    mr = jnp.max(tops, axis=0)
    lse_row = mr + jnp.log(jnp.sum(adds * jnp.exp(tops - mr[None]), axis=0))
    mc = jnp.max(tops, axis=1, keepdims=True)
    lse_col = (mc + jnp.log(jnp.sum(adds * jnp.exp(tops - mc), axis=1, keepdims=True))).reshape(16, 128)
    lane8 = iota((8, 128), 1)
    lane16 = iota((16, 128), 1)
    row_sum = jnp.sum(jnp.where(lane8 < 64, lse_row, 0.0), axis=0, keepdims=True)
    col_sum = jnp.sum(jnp.where((lane16 >= 64) & (lane16 < 96), lse_col, 0.0), axis=0, keepdims=True)
    pos_sum = jnp.sum(jnp.sum(tops, axis=0), axis=0, keepdims=True)
    total = jnp.sum(row_sum + col_sum - jnp.where(lane1 == 96, 2.0 * pos_sum, 0.0), axis=1, keepdims=True)
    lm_ref[...] = jnp.broadcast_to(total / 1024.0, (1, 128))

    def to_front(v, start):
        return pltpu.roll(v, lax.rem(128 - start, 128), 1)

    pos_front = to_front(pos_q, my_slot * 4)
    my_row = jnp.sum(jnp.where(iota((8, 128), 0) == my_line, lse_row, 0.0), axis=0, keepdims=True)
    my_col = jnp.sum(jnp.where(iota((16, 128), 0) == my_slot, lse_col, 0.0), axis=0, keepdims=True)
    lq_ref[...] = (to_front(my_row, my_slot * 4) - pos_front)
    ld_ref[...] = (to_front(my_col, 64 + my_line * 4) - pos_front)
    everyone.wait_send()


def solution(mesh):
    batch_spec = P(('replica', 'data'))

    def local_loss(q_hidden, d_hidden, w_proj, q_mask, d_mask, temperature):
        vmem = pl.BlockSpec(memory_space=pltpu.VMEM)
        hbm = pl.BlockSpec(memory_space=pltpu.HBM)
        dma = pltpu.SemaphoreType.DMA
        lq, ld, lm = pl.pallas_call(
            kernel,
            out_shape=(jax.ShapeDtypeStruct((1, 128), F32),) * 3,
            in_specs=[hbm] * 5 + [pl.BlockSpec(memory_space=pltpu.SMEM)],
            out_specs=(vmem, vmem, vmem),
            scratch_shapes=[
                pltpu.VMEM((4, 32, 768), BF16),
                pltpu.VMEM((180, 4, 768), BF16),
                pltpu.VMEM((768, 128), BF16),
                pltpu.VMEM((4, 32), jnp.int32),
                pltpu.VMEM((4, 180), jnp.int32),
                dma((8,)),
                pltpu.VMEM((736, 128), F32),
                pltpu.VMEM((16, 128, 128), BF16),
                pltpu.VMEM((4, 2, 720, 128), BF16),
                pltpu.VMEM((4, 2, 2, 8, 2048), F32),
                pltpu.VMEM((2048, 128), BF16),
                pltpu.VMEM((128, 2, 128), F32),
                dma((16,)), dma((16,)), dma((10,)), dma((10,)), dma((8,)), dma((8,)), dma, dma,
                pltpu.SemaphoreType.REGULAR,
            ],
            compiler_params=pltpu.CompilerParams(collective_id=0, has_side_effects=True,
                                                 vmem_limit_bytes=48 * 1024 * 1024),
        )(*[pltpu.with_memory_space_constraint(a, pltpu.HBM)
            for a in (q_hidden, jnp.swapaxes(d_hidden, 0, 1), w_proj, q_mask, d_mask)], temperature.reshape(1))
        return lq[0, :4], ld[0, :4], lm[0, :1]

    return jax.shard_map(local_loss, mesh=mesh, in_specs=(batch_spec, batch_spec, P(), batch_spec, batch_spec, P()),
                         out_specs=(batch_spec, batch_spec, P('replica')), check_vma=False)
```
